32 devices in a mesh: ctx: 4 (over y, x), fsdp: 8 (over z, core).
Axes of the slice: x: 2, y: 2, z: 4, core: 2. Of those that a mesh axis runs over, the one named last changes fastest.
Arguments:
- queries: bfloat16 [512, 3072], P('ctx', 'fsdp'), may hold values from -200 to 200, as said below
- keys: bfloat16 [512, 3072], P('ctx', 'fsdp'), may hold values from -200 to 200, as said below
- values: bfloat16 [512, 3072], P('ctx', 'fsdp'), may hold values from -6 to 6
- query_tangent: bfloat16 [512, 3072], P('ctx', 'fsdp'), may hold values from -6 to 6
- key_tangent: bfloat16 [512, 3072], P('ctx', 'fsdp'), may hold values from -6 to 6
- value_tangent: bfloat16 [512, 3072], P('ctx', 'fsdp'), may hold values from -6 to 6
- query_gain: float32 [3072], P('fsdp'), may hold values from 0.5 to 1.5
- key_gain: float32 [3072], P('fsdp'), may hold values from 0.5 to 1.5
- time_index: int32 [1], replicated, may hold values from 0 to 999
- shard_order: int32 [4], P('ctx'), may hold values from 0 to 3, each once
Outputs:
- query_grad: bfloat16 [512, 3072], P('ctx', 'fsdp')
- key_grad: bfloat16 [512, 3072], P('ctx', 'fsdp')
- value_grad: bfloat16 [512, 3072], P('ctx', 'fsdp')
- query_gain_grad: float32 [3072], P('fsdp')
- key_gain_grad: float32 [3072], P('fsdp')
The draws below stay inside these ranges and needn't reach their ends.
Inputs may be any that keep to these rules, and one draw needn't show every extreme that they name: `queries`: each sample's channels hold 24 heads of 128 channels in order. `keys`: laid out as the queries. `shard_order`: each block index appears once.
All inputs are finite; a program needn't handle non-finite values.
Results may differ from the reference program's by a relative error of at most 0.024.
Values may be sent and summed in bfloat16 or wider, within the bound.
No kernel may reach another device: no remote copies, remote signals or barrier semaphores. Data moves between devices by JAX's collectives and lax.ppermute only.
A program may use at most 64 MiB of HBM per device.

```python
import math
import jax
import jax.numpy as jnp
from jax import lax

TOK_DEV = 128
HD = 128
STEPS = 1000
HEADS = 24
CHANNELS = 3072
SAMPLES = 1
SEQ = 512
N_CTX = 4


def drawn_pair(key):
    width_all = SAMPLES * CHANNELS
    query_base = jax.random.truncated_normal(jax.random.fold_in(key, 101), -6.0, 6.0, (SEQ, width_all), jnp.float32)
    key_base = jax.random.truncated_normal(jax.random.fold_in(key, 102), -6.0, 6.0, (SEQ, width_all), jnp.float32)
    return (query_base, key_base)


def draw_queries(key, part):
    return drawn_pair(key)[0].astype(jnp.bfloat16)


def draw_keys(key, part):
    return drawn_pair(key)[1].astype(jnp.bfloat16)


def steps_of(key, shape, pieces, low, high):
    def one(axis_at, parts):
        heights = jax.random.uniform(jax.random.fold_in(jax.random.fold_in(key, 6), axis_at), (parts,), jnp.float32, low / len(pieces), high / len(pieces))
        return jnp.repeat(jnp.exp(heights), shape[axis_at] // parts).reshape((-1,) + (1,) * (len(shape) - axis_at - 1))

    level = one(*pieces[0])
    for cut in pieces[1:]:
        level = level * one(*cut)
    return level


def gaussian(own_key, dims, width, limit, cuts=(), held_as=jnp.bfloat16):
    gain = steps_of(own_key, dims, cuts, -0.22, 0.18) if cuts else 1.0
    entries = jax.random.normal(own_key, dims, jnp.float32) * width * gain
    return jnp.minimum(jnp.maximum(entries, -limit), limit).astype(held_as)


def setup_inputs(seed: int = 0) -> dict:
    splits = jax.random.split(jax.random.key(seed), 11)
    queries = draw_queries(jax.random.fold_in(splits[10], 71), 0)
    keys = draw_keys(jax.random.fold_in(splits[10], 71), 0)
    values = gaussian(splits[2], (SEQ, SAMPLES * CHANNELS), 1.0, 6.0, ((0, 4), (1, 8)))
    query_tangent = gaussian(splits[3], (SEQ, SAMPLES * CHANNELS), 1.0, 6.0, ((0, 4), (1, 8)))
    key_tangent = gaussian(splits[4], (SEQ, SAMPLES * CHANNELS), 1.0, 6.0, ((0, 4), (1, 8)))
    value_tangent = gaussian(splits[5], (SEQ, SAMPLES * CHANNELS), 1.0, 6.0, ((0, 4), (1, 8)))
    query_gain = jnp.clip(1.0 + 0.1 * jax.random.normal(splits[6], (CHANNELS,), jnp.float32), 0.5, 1.5)
    key_gain = jnp.clip(1.0 + 0.1 * jax.random.normal(splits[7], (CHANNELS,), jnp.float32), 0.5, 1.5)
    time_index = jax.random.randint(splits[8], (SAMPLES,), 0, STEPS).astype(jnp.int32)
    shard_order = jax.random.permutation(splits[9], N_CTX).astype(jnp.int32)
    return {"queries": queries, "keys": keys, "values": values, "query_tangent": query_tangent, "key_tangent": key_tangent, "value_tangent": value_tangent, "query_gain": query_gain, "key_gain": key_gain, "time_index": time_index, "shard_order": shard_order}


eps_norm = 1e-06
loss_scale = 256.0
rope_base = 10000.0
floor_term = 0.1

def rope_tables(shard_order):
    row_ids = jnp.arange(SEQ, dtype=jnp.int32)
    block_ids = row_ids // TOK_DEV
    onehot = (block_ids[:, None] == jnp.arange(N_CTX, dtype=jnp.int32)[None, :]).astype(jnp.int32)
    starts = lax.optimization_barrier(jnp.sum(onehot * shard_order[None, :].astype(jnp.int32), axis=1)) * TOK_DEV
    places = (starts + row_ids % TOK_DEV).astype(jnp.float32)
    freqs = rope_base ** (-jnp.arange(HD // 2, dtype=jnp.float32) / (HD // 2))
    angles = places[:, None] * freqs[None, :]
    return (jnp.cos(angles), jnp.sin(angles))

def rotate(field, cos_table, sin_table, turn_sign):
    half_width = field.shape[-1] // 2
    first_half = field[..., :half_width]
    second_half = field[..., half_width:]
    return jnp.concatenate([first_half * cos_table - turn_sign * second_half * sin_table, turn_sign * first_half * sin_table + second_half * cos_table], axis=-1)

def normalize(field, field_tan, gain_vec):
    inv_rms = lax.rsqrt(lax.optimization_barrier(jnp.mean(field * field, axis=-1, keepdims=True)) + eps_norm)
    cross = lax.optimization_barrier(jnp.mean(field * field_tan, axis=-1, keepdims=True))
    normed = field * inv_rms * gain_vec
    normed_tan = (field_tan * inv_rms - field * inv_rms ** 3 * cross) * gain_vec
    return (normed, normed_tan, inv_rms)

def denormalize(field, inv_rms, gain_vec, grad_y):
    scaled = gain_vec * grad_y
    cross = lax.optimization_barrier(jnp.mean(field * scaled, axis=-1, keepdims=True))
    backed = inv_rms * scaled - field * inv_rms ** 3 * cross
    gain_grad = lax.optimization_barrier(jnp.sum(grad_y * field * inv_rms, axis=(0, 1)))
    return (backed, gain_grad)

def forward_pair(group):
    query_blk, key_blk, value_blk, qtan_blk, ktan_blk, vtan_blk = group
    inv_root = HD ** (-0.5)
    scores = jnp.dot(query_blk, key_blk.T, preferred_element_type=jnp.float32) * inv_root
    slopes = (jnp.dot(qtan_blk, key_blk.T, preferred_element_type=jnp.float32) + jnp.dot(query_blk, ktan_blk.T, preferred_element_type=jnp.float32)) * inv_root
    peak = lax.optimization_barrier(jnp.max(scores, axis=1, keepdims=True))
    weights = jnp.exp(scores - peak)
    totals = lax.optimization_barrier(jnp.sum(weights, axis=1, keepdims=True))
    tilted = weights * slopes
    weights_b = weights.astype(jnp.bfloat16)
    tilted_b = tilted.astype(jnp.bfloat16)
    numer = jnp.dot(weights_b, value_blk, preferred_element_type=jnp.float32)
    numer_tan = jnp.dot(weights_b, vtan_blk, preferred_element_type=jnp.float32) + jnp.dot(tilted_b, value_blk, preferred_element_type=jnp.float32)
    tilt = lax.optimization_barrier(jnp.sum(tilted, axis=1, keepdims=True))
    output = numer / totals
    output_tan = numer_tan / totals - tilt / totals * output
    return (output, output_tan, peak + jnp.log(totals))

def backward_pair(group):
    query_blk, key_blk, value_blk, cot_blk, logsum, drift = group
    inv_root = HD ** (-0.5)
    scores = jnp.dot(query_blk, key_blk.T, preferred_element_type=jnp.float32) * inv_root
    probs = jnp.exp(scores - logsum)
    probs_b = probs.astype(jnp.bfloat16)
    dvalue = jnp.dot(probs_b.T, cot_blk, preferred_element_type=jnp.float32)
    dprobs = jnp.dot(cot_blk, value_blk.T, preferred_element_type=jnp.float32)
    dscore = (probs * (dprobs - drift) * inv_root).astype(jnp.bfloat16)
    dquery = jnp.dot(dscore, key_blk, preferred_element_type=jnp.float32)
    dkey = jnp.dot(dscore.T, query_blk, preferred_element_type=jnp.float32)
    return (dquery, dkey, dvalue)

def reference(queries, keys, values, query_tangent, key_tangent, value_tangent, query_gain, key_gain, time_index, shard_order):
    cos_table, sin_table = rope_tables(shard_order)
    cos_four = cos_table[:, None, None, :]
    sin_four = sin_table[:, None, None, :]

    def spread(array):
        return array.astype(jnp.float32).reshape(SEQ, SAMPLES, CHANNELS)

    def heads_of(array):
        return array.reshape(SEQ, SAMPLES, HEADS, HD)

    def to_pairs(array):
        return jnp.transpose(array, (1, 2, 0, 3)).reshape(SAMPLES * HEADS, SEQ, array.shape[-1])

    def from_pairs(array):
        return jnp.transpose(array.reshape(SAMPLES, HEADS, SEQ, array.shape[-1]), (2, 0, 1, 3))
    query_x = spread(queries)
    key_x = spread(keys)
    query_y, query_yt, query_r = normalize(query_x, spread(query_tangent), query_gain.astype(jnp.float32))
    key_y, key_yt, key_r = normalize(key_x, spread(key_tangent), key_gain.astype(jnp.float32))
    query_n = rotate(heads_of(query_y), cos_four, sin_four, 1.0).astype(jnp.bfloat16)
    query_nt = rotate(heads_of(query_yt), cos_four, sin_four, 1.0).astype(jnp.bfloat16)
    key_n = rotate(heads_of(key_y), cos_four, sin_four, 1.0).astype(jnp.bfloat16)
    key_nt = rotate(heads_of(key_yt), cos_four, sin_four, 1.0).astype(jnp.bfloat16)
    value_h = heads_of(values)
    value_ht = heads_of(value_tangent)
    outputs, output_tan, logsum = lax.map(forward_pair, (to_pairs(query_n), to_pairs(key_n), to_pairs(value_h), to_pairs(query_nt), to_pairs(key_nt), to_pairs(value_ht)))
    outputs = from_pairs(outputs)
    output_tan = from_pairs(output_tan)
    logsum = from_pairs(logsum)
    angle_t = 0.5 * math.pi * (time_index.astype(jnp.float32) + 0.5) / STEPS
    coef_out = (jnp.sin(angle_t) * jnp.cos(angle_t))[None, :, None, None]
    coef_tan = (jnp.cos(angle_t) ** 2)[None, :, None, None]
    raw_target = coef_out * outputs + coef_tan * output_tan
    level = jnp.sqrt(lax.optimization_barrier(jnp.mean(raw_target * raw_target, axis=(2, 3), keepdims=True)))
    cotangent = (loss_scale * raw_target / (level + floor_term)).astype(jnp.bfloat16)
    drift = lax.optimization_barrier(jnp.sum(cotangent.astype(jnp.float32) * outputs, axis=-1, keepdims=True))
    dquery, dkey, dvalue = lax.map(backward_pair, (to_pairs(query_n), to_pairs(key_n), to_pairs(value_h), to_pairs(cotangent), to_pairs(logsum), to_pairs(drift)))
    query_dy = rotate(from_pairs(dquery), cos_four, sin_four, -1.0).reshape(SEQ, SAMPLES, CHANNELS)
    key_dy = rotate(from_pairs(dkey), cos_four, sin_four, -1.0).reshape(SEQ, SAMPLES, CHANNELS)
    query_back, query_gain_grad = denormalize(query_x, query_r, query_gain.astype(jnp.float32), query_dy)
    key_back, key_gain_grad = denormalize(key_x, key_r, key_gain.astype(jnp.float32), key_dy)
    query_grad = query_back.reshape(SEQ, SAMPLES * CHANNELS).astype(jnp.bfloat16)
    key_grad = key_back.reshape(SEQ, SAMPLES * CHANNELS).astype(jnp.bfloat16)
    value_grad = from_pairs(dvalue).reshape(SEQ, SAMPLES * CHANNELS).astype(jnp.bfloat16)
    return (query_grad, key_grad, value_grad, query_gain_grad, key_gain_grad)
```

```python
import functools
import math

import jax
import jax.numpy as jnp
import numpy as np
from jax import lax
from jax.experimental import pallas as pl
from jax.experimental.pallas import tpu as pltpu
from jax.sharding import PartitionSpec as P

HD = 128
STEPS = 1000

eps_norm = 1e-06
loss_scale = 256.0
rope_base = 10000.0
floor_term = 0.1

BOTH = ("ctx", "fsdp")
F32 = jnp.float32
BF16 = jnp.bfloat16
ORDER_ROWS = 16

NT = (((1,), (1,)), ((), ()))
TN = (((0,), (0,)), ((), ()))
NN = (((1,), (0,)), ((), ()))


def mm(lhs, rhs, dims):
    return lax.dot_general(lhs, rhs, dims, preferred_element_type=F32)


def eye_mask(size):
    rows = lax.broadcasted_iota(jnp.int32, (size, size), 0)
    return rows == lax.broadcasted_iota(jnp.int32, (size, size), 1)


def as_row(column):
    return jnp.sum(jnp.where(eye_mask(column.shape[0]), column, 0.0), axis=0, keepdims=True)


def as_column(row):
    return jnp.sum(jnp.where(eye_mask(row.shape[1]), row, 0.0), axis=1, keepdims=True)


def hosted_head(ctx_id, fsdp_id, n_ctx):
    return (ctx_id + n_ctx - fsdp_id % n_ctx) % n_ctx


def turn(field, cos_t, sin_t):
    return field * cos_t + pltpu.roll(field, HD // 2, 1) * sin_t


def sample_sum(ref, ctx_id, n_fsdp, head_split):
    start = ctx_id * n_fsdp + (lax.axis_index("fsdp") // head_split) * head_split
    return jnp.sum(ref[pl.ds(start, head_split)], axis=0)


def norm_scales(stats, channels):
    mean = stats * (1.0 / channels)
    inv = lax.rsqrt(mean[0:2] + eps_norm)
    inv_q, inv_k = as_column(inv[0:1]), as_column(inv[1:2])
    tilt = inv * inv * inv * mean[2:4]
    return inv_q, inv_k, as_column(tilt[0:1]), as_column(tilt[1:2])


def pack_kernel(n_ctx, heads, order_ref, q_ref, k_ref, v_ref, qt_ref, kt_ref, vt_ref, *outs):
    stats_ref, block_refs = outs[0], outs[1:]
    ctx_id, fsdp_id = lax.axis_index("ctx"), lax.axis_index("fsdp")
    rows = q_ref.shape[0]
    order = jnp.full((ORDER_ROWS, HD), order_ref[0].astype(F32), F32).astype(BF16)
    for dist, block in enumerate(block_refs):
        head = jnp.minimum(hosted_head(ctx_id ^ dist, fsdp_id, n_ctx), heads - 1)
        lanes = pl.ds(pl.multiple_of(head * HD, HD), HD)
        for at, ref in enumerate((q_ref, k_ref, v_ref, qt_ref, kt_ref, vt_ref)):
            block[at * rows : (at + 1) * rows, :] = ref[:, lanes]
        block[6 * rows :, :] = order
    q, k = q_ref[...].astype(F32), k_ref[...].astype(F32)
    qt, kt = qt_ref[...].astype(F32), kt_ref[...].astype(F32)
    sums = jnp.concatenate(
        [as_row(jnp.sum(p, axis=1, keepdims=True)) for p in (q * q, k * k, q * qt, k * kt)], axis=0
    )
    stats_ref[...] = jnp.broadcast_to(sums[None], stats_ref.shape)


def forward_kernel(n_ctx, n_fsdp, heads, channels, *refs):
    stats_ref, gains_ref, table_ref, coef_ref = refs[:4]
    block_refs = refs[4 : 4 + n_ctx]
    energy_ref, qcat_ref, kcat_ref, vcat_ref, out_ref, goal_ref, lse_ref, turn_ref = refs[4 + n_ctx :]
    ctx_id, fsdp_id = lax.axis_index("ctx"), lax.axis_index("fsdp")
    head = hosted_head(ctx_id, fsdp_id, n_ctx)
    active = head < heads
    gain_q, gain_k = gains_ref[0:1], gains_ref[1:2]
    rows = (block_refs[0].shape[0] - ORDER_ROWS) // 6
    inv_root = HD ** (-0.5)
    for dist, block in enumerate(block_refs):
        here = slice(dist * rows, (dist + 1) * rows)
        stats = sample_sum(stats_ref, ctx_id ^ dist, n_fsdp, channels // (heads * HD))
        inv_q, inv_k, tilt_q, tilt_k = norm_scales(stats, channels)
        order = block[6 * rows : 6 * rows + 1, :].astype(F32)
        both = table_ref[0:rows, :]
        for other in range(1, n_ctx):
            both = jnp.where(order == float(other), table_ref[other * rows : (other + 1) * rows, :], both)
        swapped = pltpu.roll(both, HD // 2, 1)
        low = lax.broadcasted_iota(jnp.int32, (rows, HD), 1) < HD // 2
        cos_t = jnp.where(low, both, swapped)
        sin_t = jnp.where(low, -swapped, both)
        turn_ref[here, 0:HD] = cos_t
        turn_ref[here, HD:] = sin_t

        def part(at):
            return block[at * rows : (at + 1) * rows, :]

        q, k = part(0).astype(F32), part(1).astype(F32)
        qt, kt = part(3).astype(F32), part(4).astype(F32)
        qcat_ref[here, HD:] = turn(q * inv_q * gain_q, cos_t, sin_t).astype(BF16)
        qcat_ref[here, 0:HD] = turn((qt * inv_q - q * tilt_q) * gain_q, cos_t, sin_t).astype(BF16)
        kcat_ref[here, 0:HD] = turn(k * inv_k * gain_k, cos_t, sin_t).astype(BF16)
        kcat_ref[here, HD:] = turn((kt * inv_k - k * tilt_k) * gain_k, cos_t, sin_t).astype(BF16)
        vcat_ref[here, 0:HD] = part(2)
        vcat_ref[here, HD:] = part(5)
    for dist in range(n_ctx):
        here = slice(dist * rows, (dist + 1) * rows)
        scores = mm(qcat_ref[here, HD:], kcat_ref[:, 0:HD], NT) * inv_root
        slopes = mm(qcat_ref[here, :], kcat_ref[...], NT) * inv_root
        peak = jnp.max(scores, axis=1, keepdims=True)
        weights = jnp.exp(scores - peak)
        totals = jnp.sum(weights, axis=1, keepdims=True)
        tilted = weights * slopes
        numer = mm(weights.astype(BF16), vcat_ref[...], NN)
        numer_tan = numer[:, HD:] + mm(tilted.astype(BF16), vcat_ref[:, 0:HD], NN)
        tilt = jnp.sum(tilted, axis=1, keepdims=True)
        output = numer[:, 0:HD] / totals
        output_tan = numer_tan / totals - (tilt / totals) * output
        goal = coef_ref[0:1] * output + coef_ref[1:2] * output_tan
        out_ref[here, :] = output
        goal_ref[here, :] = goal
        lse_ref[here, :] = jnp.broadcast_to(peak + jnp.log(totals), (rows, HD))
        row = as_row(jnp.sum(goal * goal, axis=1, keepdims=True))
        energy_ref[0, pl.ds(ctx_id ^ dist, 1), :] = jnp.where(active, row, 0.0)
    first = energy_ref[0]
    for at in range(1, energy_ref.shape[0]):
        energy_ref[at] = first


def backward_kernel(n_ctx, n_fsdp, heads, channels, *refs):
    stats_ref, energy_ref, gains_ref, qcat_ref, kcat_ref, vcat_ref = refs[:6]
    out_ref, goal_ref, lse_ref, turn_ref = refs[6:10]
    block_refs = refs[10 : 10 + n_ctx]
    cross_ref = refs[10 + n_ctx]
    back_refs = refs[11 + n_ctx : 11 + 2 * n_ctx]
    probs_ref, dscore_ref, cot_ref = refs[11 + 2 * n_ctx :]
    ctx_id, fsdp_id = lax.axis_index("ctx"), lax.axis_index("fsdp")
    active = hosted_head(ctx_id, fsdp_id, n_ctx) < heads
    head_split = channels // (heads * HD)
    sample = fsdp_id // head_split
    gain_q, gain_k = gains_ref[0:1], gains_ref[1:2]
    rows = (block_refs[0].shape[0] - ORDER_ROWS) // 6
    inv_root = HD ** (-0.5)
    energy = jnp.zeros((n_ctx, rows), F32)
    for ctx_at in range(n_ctx):
        energy = energy + jnp.sum(energy_ref[pl.ds(ctx_at * n_fsdp + sample * head_split, head_split)], axis=0)
    level = loss_scale / (jnp.sqrt(energy * (1.0 / channels)) + floor_term)
    block_ids = lax.broadcasted_iota(jnp.int32, (n_ctx, rows), 0)
    gain_q_sum = jnp.zeros((1, HD), F32)
    gain_k_sum = jnp.zeros((1, HD), F32)
    crosses = []
    for dist in range(n_ctx):
        here = slice(dist * rows, (dist + 1) * rows)
        owner = ctx_id ^ dist
        scale = as_column(jnp.sum(jnp.where(block_ids == owner, level, 0.0), axis=0, keepdims=True))
        output = out_ref[here, :]
        cot = (scale * goal_ref[here, :]).astype(BF16)
        drift = jnp.sum(cot.astype(F32) * output, axis=1, keepdims=True)
        scores = mm(qcat_ref[here, HD:], kcat_ref[:, 0:HD], NT) * inv_root
        probs = jnp.exp(scores - lse_ref[here, 0:1])
        dprobs = mm(cot, vcat_ref[:, 0:HD], NT)
        dscore = (probs * (dprobs - drift) * inv_root).astype(BF16)
        probs_ref[here, :] = probs.astype(BF16)
        dscore_ref[here, :] = dscore
        cot_ref[here, :] = cot
        dquery = mm(dscore, kcat_ref[:, 0:HD], NN)
        inv_q = norm_scales(sample_sum(stats_ref, owner, n_fsdp, head_split), channels)[0]
        x = block_refs[dist][0:rows, :].astype(F32)
        dy = turn(dquery, turn_ref[here, 0:HD], -turn_ref[here, HD:])
        grown = gain_q * dy
        back_refs[dist][0:rows, :] = grown.astype(BF16)
        crosses.append(as_row(jnp.sum(x * grown, axis=1, keepdims=True)))
        gain_q_sum = gain_q_sum + jnp.sum(dy * x * inv_q, axis=0, keepdims=True)
    for dist in range(n_ctx):
        here = slice(dist * rows, (dist + 1) * rows)
        owner = ctx_id ^ dist
        back_refs[dist][2 * rows : 3 * rows, :] = mm(probs_ref[:, here], cot_ref[...], TN).astype(BF16)
        dkey = mm(dscore_ref[:, here], qcat_ref[:, HD:], TN)
        inv_k = norm_scales(sample_sum(stats_ref, owner, n_fsdp, head_split), channels)[1]
        x = block_refs[dist][rows : 2 * rows, :].astype(F32)
        dy = turn(dkey, turn_ref[here, 0:HD], -turn_ref[here, HD:])
        grown = gain_k * dy
        back_refs[dist][rows : 2 * rows, :] = grown.astype(BF16)
        cross_k = as_row(jnp.sum(x * grown, axis=1, keepdims=True))
        gain_k_sum = gain_k_sum + jnp.sum(dy * x * inv_k, axis=0, keepdims=True)
        crosses[dist] = jnp.concatenate([crosses[dist], cross_k], axis=0)
    for dist in range(n_ctx):
        sums = jnp.concatenate([crosses[dist], gain_q_sum, gain_k_sum], axis=0)
        sums = jnp.where(active, sums, 0.0)
        start = (ctx_id ^ dist) * n_fsdp
        for at in range(n_fsdp):
            cross_ref[start + at] = sums


def finish_kernel(n_ctx, n_fsdp, heads, channels, *refs):
    stats_ref, cross_ref, q_ref, k_ref = refs[:4]
    back_refs = refs[4 : 4 + n_ctx]
    dq_ref, dk_ref, dv_ref, dgain_ref = refs[4 + n_ctx :]
    ctx_id, fsdp_id = lax.axis_index("ctx"), lax.axis_index("fsdp")
    head_split = channels // (heads * HD)
    sample = fsdp_id // head_split
    rows = q_ref.shape[0]
    inv_q, inv_k, _, _ = norm_scales(sample_sum(stats_ref, ctx_id, n_fsdp, head_split), channels)
    total = jnp.zeros((4, rows), F32)
    for ctx_at in range(n_ctx):
        total = total + jnp.sum(cross_ref[pl.ds(ctx_at * n_fsdp + sample * head_split, head_split)], axis=0)
    mean = total[0:2] * (1.0 / channels)
    tilt_q = inv_q * inv_q * inv_q * as_column(mean[0:1])
    tilt_k = inv_k * inv_k * inv_k * as_column(mean[1:2])
    for dist in range(n_ctx):
        host = ctx_id ^ dist
        head = hosted_head(host, fsdp_id, n_ctx)

        @pl.when(head < heads)
        def _(dist=dist, host=host, head=head):
            back = back_refs[dist]
            lanes = pl.ds(pl.multiple_of(head * HD, HD), HD)
            h_q, h_k = back[0:rows, :].astype(F32), back[rows : 2 * rows, :].astype(F32)
            dq_ref[:, lanes] = (inv_q * h_q - q_ref[:, lanes].astype(F32) * tilt_q).astype(BF16)
            dk_ref[:, lanes] = (inv_k * h_k - k_ref[:, lanes].astype(F32) * tilt_k).astype(BF16)
            dv_ref[:, lanes] = back[2 * rows : 3 * rows, :]
            dgain_ref[:, lanes] = cross_ref[host * n_fsdp + fsdp_id, 2:4, :]


def per_device(
    queries,
    keys,
    values,
    query_tangent,
    key_tangent,
    value_tangent,
    query_gain,
    key_gain,
    time_index,
    shard_order,
):
    n_ctx, n_fsdp = lax.axis_size("ctx"), lax.axis_size("fsdp")
    n_all = n_ctx * n_fsdp
    ctx_id, fsdp_id = lax.axis_index("ctx"), lax.axis_index("fsdp")
    rows, ch_dev = queries.shape
    heads = ch_dev // HD
    channels = query_gain.shape[0] * n_fsdp
    head_split = channels // ch_dev
    seq = rows * n_ctx
    sizes = (n_ctx, n_fsdp, heads, channels)
    head = hosted_head(ctx_id, fsdp_id, n_ctx)

    vmem = pl.BlockSpec(memory_space=pltpu.VMEM)
    smem = pl.BlockSpec(memory_space=pltpu.SMEM)

    def kernel(body, ins, outs, scratch=(), flops=10**8, in_specs=None):
        return pl.pallas_call(
            body,
            out_shape=[jax.ShapeDtypeStruct(*o) for o in outs],
            in_specs=in_specs or [vmem] * len(ins),
            out_specs=[vmem] * len(outs),
            scratch_shapes=list(scratch),
            cost_estimate=pl.CostEstimate(flops=flops, bytes_accessed=2**20, transcendentals=0),
        )(*ins)

    def exchange(chunks):
        return lax.all_to_all(chunks, BOTH, 0, 0)

    def to_peers(blocks, sends):
        out = [blocks[0]]
        for dist in range(1, n_ctx):
            route = [
                (c * n_fsdp + f, (c ^ dist) * n_fsdp + f)
                for c in range(n_ctx)
                for f in range(n_fsdp)
                if sends(c, c ^ dist, f)
            ]
            out.append(lax.ppermute(blocks[dist], BOTH, route))
        return out

    places = np.arange(seq, dtype=np.float32)
    freqs = (rope_base ** (-np.arange(HD // 2) / (HD // 2))).astype(np.float32)
    angles = (places[:, None] * freqs[None, :]).astype(np.float64)
    table = jnp.asarray(np.concatenate([np.cos(angles), np.sin(angles)], axis=1).astype(np.float32))

    if channels == query_gain.shape[0] * head_split:
        gains = (query_gain, key_gain)
    else:
        gains = tuple(
            lax.dynamic_slice_in_dim(
                lax.all_gather(g, "fsdp", axis=0, tiled=True), (fsdp_id % head_split) * ch_dev, ch_dev, 0
            )
            for g in (query_gain, key_gain)
        )
    head_at = jnp.minimum(head, heads - 1) * HD
    head_gains = jnp.stack([lax.dynamic_slice_in_dim(g, head_at, HD, 0) for g in gains])

    slot_count = time_index.shape[0]
    picked = jnp.sum(
        jnp.where(jnp.arange(slot_count, dtype=jnp.int32) == fsdp_id // head_split, time_index, 0)
    )
    angle_t = 0.5 * math.pi * (picked.astype(F32) + 0.5) / STEPS
    coefs = jnp.stack([jnp.sin(angle_t) * jnp.cos(angle_t), jnp.cos(angle_t) ** 2])
    coefs = jnp.broadcast_to(coefs[:, None], (2, HD))

    block_shape = ((6 * rows + ORDER_ROWS, HD), BF16)
    stats_out, *blocks = kernel(
        functools.partial(pack_kernel, n_ctx, heads),
        (shard_order, queries, keys, values, query_tangent, key_tangent, value_tangent),
        [((n_all, 4, rows), F32)] + [block_shape] * n_ctx,
        in_specs=[smem] + [vmem] * 6,
    )
    blocks = to_peers(blocks, lambda c, peer, f: hosted_head(peer, f, n_ctx) < heads)
    stats = exchange(stats_out)

    energy_out, qcat, kcat, vcat, output, goal, lse, turns = kernel(
        functools.partial(forward_kernel, *sizes),
        (stats, head_gains, table, coefs, *blocks),
        [((n_all, n_ctx, rows), F32)]
        + [((seq, 2 * HD), BF16)] * 3
        + [((seq, HD), F32)] * 3
        + [((seq, 2 * HD), F32)],
    )
    energy = exchange(energy_out)

    cross_out, *back = kernel(
        functools.partial(backward_kernel, *sizes),
        (stats, energy, head_gains, qcat, kcat, vcat, output, goal, lse, turns, *blocks),
        [((n_all, 4, rows), F32)] + [((3 * rows, HD), BF16)] * n_ctx,
        scratch=[
            pltpu.VMEM((seq, seq), BF16),
            pltpu.VMEM((seq, seq), BF16),
            pltpu.VMEM((seq, HD), BF16),
        ],
    )
    back = to_peers(back, lambda c, peer, f: hosted_head(c, f, n_ctx) < heads)
    crosses = exchange(cross_out)

    query_grad, key_grad, value_grad, gain_grads = kernel(
        functools.partial(finish_kernel, *sizes),
        (stats, crosses, queries, keys, *back),
        [((rows, ch_dev), BF16)] * 3 + [((2, ch_dev), F32)],
    )
    if query_gain.shape[0] == ch_dev:
        query_gain_grad, key_gain_grad = gain_grads[0], gain_grads[1]
    else:
        start = (fsdp_id % head_split) * ch_dev
        placed = lax.dynamic_update_slice(jnp.zeros((2, channels), F32), gain_grads, (0, start))
        query_gain_grad, key_gain_grad = lax.psum_scatter(placed, "fsdp", scatter_dimension=1, tiled=True)
    return (query_grad, key_grad, value_grad, query_gain_grad, key_gain_grad)


def solution(mesh):
    placed = (P("ctx", "fsdp"),) * 6 + (P("fsdp"), P("fsdp"), P(), P("ctx"))
    return jax.shard_map(
        per_device,
        mesh=mesh,
        in_specs=placed,
        out_specs=(P("ctx", "fsdp"), P("ctx", "fsdp"), P("ctx", "fsdp"), P("fsdp"), P("fsdp")),
        check_vma=False,
    )
```

```python
import functools
import math

import jax
import jax.numpy as jnp
import numpy as np
from jax import lax
from jax.experimental import pallas as pl
from jax.experimental.pallas import tpu as pltpu
from jax.sharding import PartitionSpec as P


HD = 128
STEPS = 1000

eps_norm = 1e-06
loss_scale = 256.0
rope_base = 10000.0
floor_term = 0.1

BOTH = ("ctx", "fsdp")
F32 = jnp.float32
BF16 = jnp.bfloat16
ORDER_ROWS = 16

NT = (((1,), (1,)), ((), ()))
TN = (((0,), (0,)), ((), ()))
NN = (((1,), (0,)), ((), ()))


def mm(lhs, rhs, dims):
    return lax.dot_general(lhs, rhs, dims, preferred_element_type=F32)


def eye_mask(size):
    rows = lax.broadcasted_iota(jnp.int32, (size, size), 0)
    return rows == lax.broadcasted_iota(jnp.int32, (size, size), 1)


def as_row(column):
    return jnp.sum(jnp.where(eye_mask(column.shape[0]), column, 0.0), axis=0, keepdims=True)


def as_column(row):
    return jnp.sum(jnp.where(eye_mask(row.shape[1]), row, 0.0), axis=1, keepdims=True)


def hosted_head(ctx_id, fsdp_id, n_ctx):
    return (ctx_id + n_ctx - fsdp_id % n_ctx) % n_ctx


def turn(field, cos_t, sin_t):
    return field * cos_t + pltpu.roll(field, HD // 2, 1) * sin_t


def head_lanes(head, heads):
    return pl.ds(pl.multiple_of(jnp.minimum(head, heads - 1) * HD, HD), HD)


def norm_scales(stats, channels):
    mean = stats * (1.0 / channels)
    inv = lax.rsqrt(mean[0:2] + eps_norm)
    inv_q, inv_k = as_column(inv[0:1]), as_column(inv[1:2])
    tilt = inv * inv * inv * mean[2:4]
    return inv_q, inv_k, as_column(tilt[0:1]), as_column(tilt[1:2])


def pack_kernel(n_ctx, heads, *refs):
    order_hbm, gain_hbms, field_hbms = refs[0], refs[1:3], refs[3:9]
    stats_ref, gain_refs, block_refs = refs[9], refs[10:12], refs[12 : 12 + n_ctx]
    order_ref, line_refs, field_refs, sems = refs[12 + n_ctx], refs[13 + n_ctx : 15 + n_ctx], refs[15 + n_ctx : -1], refs[-1]
    sources = (*field_hbms, order_hbm, *gain_hbms)
    targets = (*field_refs, order_ref, *line_refs)
    copies = [pltpu.make_async_copy(a, b, sems.at[at]) for at, (a, b) in enumerate(zip(sources, targets))]
    for copy in copies:
        copy.start()
    ctx_id, fsdp_id = lax.axis_index("ctx"), lax.axis_index("fsdp")
    rows = field_refs[0].shape[0]
    for copy in copies:
        copy.wait()
    order = jnp.full((ORDER_ROWS, HD), order_ref[0].astype(F32), F32).astype(BF16)
    for dist, block in enumerate(block_refs):
        lanes = head_lanes(hosted_head(ctx_id ^ dist, fsdp_id, n_ctx), heads)
        for at, ref in enumerate(field_refs):
            block[at * rows : (at + 1) * rows, :] = ref[:, lanes]
        block[6 * rows :, :] = order
    q, k, qt, kt = (field_refs[at][...].astype(F32) for at in (0, 1, 3, 4))
    for at, product in enumerate((q * q, k * k, q * qt, k * kt)):
        stats_ref[at : at + 1, :] = as_row(jnp.sum(product, axis=1, keepdims=True))
    for gain_ref, line_ref in zip(gain_refs, line_refs):
        gain_ref[...] = line_ref[...].reshape(gain_ref.shape)


def forward_kernel(n_ctx, n_fsdp, heads, channels, *refs):
    time_ref, gain_q_ref, gain_k_ref, table_ref = refs[:4]
    block_refs = refs[4 : 4 + n_ctx]
    stats_refs = refs[4 + n_ctx : 4 + 2 * n_ctx]
    energy_ref, qcat_ref, kcat_ref, vcat_ref, out_ref, goal_ref, lse_ref, turn_ref = refs[4 + 2 * n_ctx : -2]
    slots_ref, sem = refs[-2:]
    copy = pltpu.make_async_copy(time_ref, slots_ref, sem)
    copy.start()
    ctx_id, fsdp_id = lax.axis_index("ctx"), lax.axis_index("fsdp")
    head = hosted_head(ctx_id, fsdp_id, n_ctx)
    active = head < heads
    lanes = head_lanes(head, heads)
    gain_q, gain_k = gain_q_ref[:, lanes], gain_k_ref[:, lanes]
    rows = (block_refs[0].shape[0] - ORDER_ROWS) // 6
    inv_root = HD ** (-0.5)
    for dist, block in enumerate(block_refs):
        here = slice(dist * rows, (dist + 1) * rows)
        inv_q, inv_k, tilt_q, tilt_k = norm_scales(stats_refs[dist][...], channels)
        order = block[6 * rows : 6 * rows + 1, :].astype(F32)
        both = table_ref[0:rows, :]
        for other in range(1, n_ctx):
            both = jnp.where(order == float(other), table_ref[other * rows : (other + 1) * rows, :], both)
        swapped = pltpu.roll(both, HD // 2, 1)
        low = lax.broadcasted_iota(jnp.int32, (rows, HD), 1) < HD // 2
        cos_t = jnp.where(low, both, swapped)
        sin_t = jnp.where(low, -swapped, both)
        turn_ref[here, 0:HD] = cos_t
        turn_ref[here, HD:] = sin_t

        def part(at):
            return block[at * rows : (at + 1) * rows, :]

        q, k = part(0).astype(F32), part(1).astype(F32)
        qt, kt = part(3).astype(F32), part(4).astype(F32)
        qcat_ref[here, HD:] = turn(q * inv_q * gain_q, cos_t, sin_t).astype(BF16)
        qcat_ref[here, 0:HD] = turn((qt * inv_q - q * tilt_q) * gain_q, cos_t, sin_t).astype(BF16)
        kcat_ref[here, 0:HD] = turn(k * inv_k * gain_k, cos_t, sin_t).astype(BF16)
        kcat_ref[here, HD:] = turn((kt * inv_k - k * tilt_k) * gain_k, cos_t, sin_t).astype(BF16)
        vcat_ref[here, 0:HD] = part(2)
        vcat_ref[here, HD:] = part(5)
    copy.wait()
    picked = slots_ref[fsdp_id // (channels // (heads * HD))].astype(F32)
    angle_t = jnp.full((8, HD), 0.5 * math.pi * (picked + 0.5) / STEPS)
    coef_out = (jnp.sin(angle_t) * jnp.cos(angle_t))[0:1]
    coef_tan = (jnp.cos(angle_t) ** 2)[0:1]
    for dist in range(n_ctx):
        here = slice(dist * rows, (dist + 1) * rows)
        scores = mm(qcat_ref[here, HD:], kcat_ref[:, 0:HD], NT) * inv_root
        slopes = mm(qcat_ref[here, :], kcat_ref[...], NT) * inv_root
        peak = jnp.max(scores, axis=1, keepdims=True)
        weights = jnp.exp(scores - peak)
        totals = jnp.sum(weights, axis=1, keepdims=True)
        tilted = weights * slopes
        numer = mm(weights.astype(BF16), vcat_ref[...], NN)
        numer_tan = numer[:, HD:] + mm(tilted.astype(BF16), vcat_ref[:, 0:HD], NN)
        tilt = jnp.sum(tilted, axis=1, keepdims=True)
        output = numer[:, 0:HD] / totals
        output_tan = numer_tan / totals - (tilt / totals) * output
        goal = coef_out * output + coef_tan * output_tan
        out_ref[here, :] = output
        goal_ref[here, :] = goal
        lse_ref[here, :] = jnp.broadcast_to(peak + jnp.log(totals), (rows, HD))
        row = as_row(jnp.sum(goal * goal, axis=1, keepdims=True))
        energy_ref[0, pl.ds(ctx_id ^ dist, 1), :] = jnp.where(active, row, 0.0)
    first = energy_ref[0]
    for at in range(1, energy_ref.shape[0]):
        energy_ref[at] = first


def backward_kernel(n_ctx, n_fsdp, heads, channels, *refs):
    energy_ref, gain_q_ref, gain_k_ref, qcat_ref, kcat_ref, vcat_ref = refs[:6]
    out_ref, goal_ref, lse_ref, turn_ref = refs[6:10]
    block_refs = refs[10 : 10 + n_ctx]
    stats_refs = refs[10 + n_ctx : 10 + 2 * n_ctx]
    cross_ref = refs[10 + 2 * n_ctx]
    back_refs = refs[11 + 2 * n_ctx : 11 + 3 * n_ctx]
    probs_ref, dscore_ref, cot_ref = refs[11 + 3 * n_ctx :]
    ctx_id, fsdp_id = lax.axis_index("ctx"), lax.axis_index("fsdp")
    head = hosted_head(ctx_id, fsdp_id, n_ctx)
    active = head < heads
    head_split = channels // (heads * HD)
    sample = fsdp_id // head_split
    lanes = head_lanes(head, heads)
    gain_q, gain_k = gain_q_ref[:, lanes], gain_k_ref[:, lanes]
    rows = (block_refs[0].shape[0] - ORDER_ROWS) // 6
    inv_root = HD ** (-0.5)
    energy = jnp.zeros((n_ctx, rows), F32)
    for ctx_at in range(n_ctx):
        energy = energy + jnp.sum(energy_ref[pl.ds(ctx_at * n_fsdp + sample * head_split, head_split)], axis=0)
    level = loss_scale / (jnp.sqrt(energy * (1.0 / channels)) + floor_term)
    block_ids = lax.broadcasted_iota(jnp.int32, (n_ctx, rows), 0)
    gain_q_sum = jnp.zeros((1, HD), F32)
    gain_k_sum = jnp.zeros((1, HD), F32)
    crosses = []
    for dist in range(n_ctx):
        here = slice(dist * rows, (dist + 1) * rows)
        owner = ctx_id ^ dist
        scale = as_column(jnp.sum(jnp.where(block_ids == owner, level, 0.0), axis=0, keepdims=True))
        output = out_ref[here, :]
        cot = (scale * goal_ref[here, :]).astype(BF16)
        drift = jnp.sum(cot.astype(F32) * output, axis=1, keepdims=True)
        scores = mm(qcat_ref[here, HD:], kcat_ref[:, 0:HD], NT) * inv_root
        probs = jnp.exp(scores - lse_ref[here, 0:1])
        dprobs = mm(cot, vcat_ref[:, 0:HD], NT)
        dscore = (probs * (dprobs - drift) * inv_root).astype(BF16)
        probs_ref[here, :] = probs.astype(BF16)
        dscore_ref[here, :] = dscore
        cot_ref[here, :] = cot
        dquery = mm(dscore, kcat_ref[:, 0:HD], NN)
        inv_q = norm_scales(stats_refs[dist][...], channels)[0]
        x = block_refs[dist][0:rows, :].astype(F32)
        dy = turn(dquery, turn_ref[here, 0:HD], -turn_ref[here, HD:])
        grown = gain_q * dy
        back_refs[dist][0:rows, :] = grown.astype(BF16)
        crosses.append(as_row(jnp.sum(x * grown, axis=1, keepdims=True)))
        gain_q_sum = gain_q_sum + jnp.sum(dy * x * inv_q, axis=0, keepdims=True)
    for dist in range(n_ctx):
        here = slice(dist * rows, (dist + 1) * rows)
        back_refs[dist][2 * rows : 3 * rows, :] = mm(probs_ref[:, here], cot_ref[...], TN).astype(BF16)
        dkey = mm(dscore_ref[:, here], qcat_ref[:, HD:], TN)
        inv_k = norm_scales(stats_refs[dist][...], channels)[1]
        x = block_refs[dist][rows : 2 * rows, :].astype(F32)
        dy = turn(dkey, turn_ref[here, 0:HD], -turn_ref[here, HD:])
        grown = gain_k * dy
        back_refs[dist][rows : 2 * rows, :] = grown.astype(BF16)
        cross_k = as_row(jnp.sum(x * grown, axis=1, keepdims=True))
        gain_k_sum = gain_k_sum + jnp.sum(dy * x * inv_k, axis=0, keepdims=True)
        crosses[dist] = jnp.concatenate([crosses[dist], cross_k], axis=0)
    for dist in range(n_ctx):
        sums = jnp.concatenate([crosses[dist], gain_q_sum, gain_k_sum], axis=0)
        sums = jnp.where(active, sums, 0.0)
        start = (ctx_id ^ dist) * n_fsdp
        for at in range(n_fsdp):
            cross_ref[start + at] = sums


def finish_kernel(n_ctx, n_fsdp, heads, channels, *refs):
    stats_ref, cross_ref, q_ref, k_ref = refs[:4]
    back_refs = refs[4 : 4 + n_ctx]
    dq_ref, dk_ref, dv_ref, dgain_q_ref, dgain_k_ref, gain_q_ref, gain_k_ref = refs[4 + n_ctx :]
    ctx_id, fsdp_id = lax.axis_index("ctx"), lax.axis_index("fsdp")
    head_split = channels // (heads * HD)
    sample = fsdp_id // head_split
    rows = q_ref.shape[0]
    inv_q, inv_k, _, _ = norm_scales(stats_ref[...], channels)
    total = jnp.zeros((4, rows), F32)
    for ctx_at in range(n_ctx):
        total = total + jnp.sum(cross_ref[pl.ds(ctx_at * n_fsdp + sample * head_split, head_split)], axis=0)
    mean = total[0:2] * (1.0 / channels)
    tilt_q = inv_q * inv_q * inv_q * as_column(mean[0:1])
    tilt_k = inv_k * inv_k * inv_k * as_column(mean[1:2])
    for dist in range(n_ctx):
        host = ctx_id ^ dist
        head = hosted_head(host, fsdp_id, n_ctx)

        @pl.when(head < heads)
        def _(dist=dist, host=host, head=head):
            back = back_refs[dist]
            lanes = head_lanes(head, heads)
            h_q, h_k = back[0:rows, :].astype(F32), back[rows : 2 * rows, :].astype(F32)
            dq_ref[:, lanes] = (inv_q * h_q - q_ref[:, lanes].astype(F32) * tilt_q).astype(BF16)
            dk_ref[:, lanes] = (inv_k * h_k - k_ref[:, lanes].astype(F32) * tilt_k).astype(BF16)
            dv_ref[:, lanes] = back[2 * rows : 3 * rows, :]
            sums = cross_ref[host * n_fsdp + fsdp_id]
            gain_q_ref[:, lanes] = sums[2:3]
            gain_k_ref[:, lanes] = sums[3:4]

    dgain_q_ref[...] = gain_q_ref[...].reshape(dgain_q_ref.shape)
    dgain_k_ref[...] = gain_k_ref[...].reshape(dgain_k_ref.shape)


def per_device(
    queries,
    keys,
    values,
    query_tangent,
    key_tangent,
    value_tangent,
    query_gain,
    key_gain,
    time_index,
    shard_order,
):
    n_ctx, n_fsdp = lax.axis_size("ctx"), lax.axis_size("fsdp")
    n_all = n_ctx * n_fsdp
    fsdp_id = lax.axis_index("fsdp")
    rows, ch_dev = queries.shape
    heads = ch_dev // HD
    channels = query_gain.shape[0] * n_fsdp
    head_split = channels // ch_dev
    seq = rows * n_ctx
    sizes = (n_ctx, n_fsdp, heads, channels)

    vmem = pl.BlockSpec(memory_space=pltpu.VMEM)

    hbm = pl.BlockSpec(memory_space=pltpu.HBM)

    def kernel(body, ins, outs, scratch=(), flops=10**8, from_hbm=0):
        return pl.pallas_call(
            body,
            out_shape=[jax.ShapeDtypeStruct(*o) for o in outs],
            in_specs=[hbm] * from_hbm + [vmem] * (len(ins) - from_hbm),
            out_specs=[vmem] * len(outs),
            scratch_shapes=list(scratch),
            cost_estimate=pl.CostEstimate(flops=flops, bytes_accessed=2**20, transcendentals=0),
            compiler_params=pltpu.CompilerParams(vmem_limit_bytes=20 * 2**20 + seq * 2**13),
        )(*ins)

    def in_hbm(array):
        return pltpu.with_memory_space_constraint(array, pltpu.HBM)

    def swap(block, axis, dist):
        return lax.ppermute(block, axis, [(i, i ^ dist) for i in range(lax.axis_size(axis))])

    def sum_over_sample(block):
        block = block + swap(block, "fsdp", 1)
        return sum([swap(block, "fsdp", d) for d in range(2, head_split, 2)], block)

    def from_peers(blocks):
        out = [blocks[0]] + [None] * (n_ctx - 1)
        for dist in reversed(range(1, n_ctx)):
            out[dist] = swap(blocks[dist], "ctx", dist)
        return out

    places = np.arange(seq, dtype=np.float32)
    freqs = (rope_base ** (-np.arange(HD // 2) / (HD // 2))).astype(np.float32)
    angles = (places[:, None] * freqs[None, :]).astype(np.float64)
    table = jnp.asarray(np.concatenate([np.cos(angles), np.sin(angles)], axis=1).astype(np.float32))

    gains = (query_gain, key_gain)
    if query_gain.shape[0] != ch_dev:
        start = (fsdp_id % head_split) * ch_dev
        gains = [lax.all_gather(g, "fsdp", axis=0, tiled=True) for g in gains]
        gains = [lax.dynamic_slice_in_dim(g, start, ch_dev, 0) for g in gains]

    fields = (queries, keys, values, query_tangent, key_tangent, value_tangent)
    gains = [in_hbm(a) for a in gains]
    fields = [in_hbm(a) for a in fields]
    part, gain_q, gain_k, *blocks = kernel(
        functools.partial(pack_kernel, n_ctx, heads),
        (shard_order, *gains, *fields),
        [((4, rows), F32)] + [((1, ch_dev), F32)] * 2 + [((6 * rows + ORDER_ROWS, HD), BF16)] * n_ctx,
        scratch=[pltpu.SMEM((1,), jnp.int32)]
        + [pltpu.VMEM((ch_dev,), F32)] * 2
        + [pltpu.VMEM((rows, ch_dev), BF16)] * 6
        + [pltpu.SemaphoreType.DMA((9,))],
        from_hbm=9,
    )
    gains = (gain_q, gain_k)
    blocks = from_peers(blocks)
    stats = from_peers([sum_over_sample(part)] * n_ctx)

    energy_out, qcat, kcat, vcat, output, goal, lse, turns = kernel(
        functools.partial(forward_kernel, *sizes),
        (time_index, *gains, table, *blocks, *stats),
        [((n_all, n_ctx, rows), F32)]
        + [((seq, 2 * HD), BF16)] * 3
        + [((seq, HD), F32)] * 3
        + [((seq, 2 * HD), F32)],
        scratch=[pltpu.SMEM(time_index.shape, jnp.int32), pltpu.SemaphoreType.DMA],
        from_hbm=1,
    )
    energy = lax.all_to_all(energy_out, BOTH, 0, 0)

    cross_out, *back = kernel(
        functools.partial(backward_kernel, *sizes),
        (energy, *gains, qcat, kcat, vcat, output, goal, lse, turns, *blocks, *stats),
        [((n_all, 4, rows), F32)] + [((3 * rows, HD), BF16)] * n_ctx,
        scratch=[
            pltpu.VMEM((seq, seq), BF16),
            pltpu.VMEM((seq, seq), BF16),
            pltpu.VMEM((seq, HD), BF16),
        ],
    )
    back = from_peers(back)
    crosses = lax.all_to_all(cross_out, BOTH, 0, 0)

    query_grad, key_grad, value_grad, *gain_grads = kernel(
        functools.partial(finish_kernel, *sizes),
        (stats[0], crosses, queries, keys, *back),
        [((rows, ch_dev), BF16)] * 3 + [((ch_dev,), F32)] * 2,
        scratch=[pltpu.VMEM((1, ch_dev), F32)] * 2,
    )
    if query_gain.shape[0] != ch_dev:
        placed = [
            lax.dynamic_update_slice_in_dim(jnp.zeros((channels,), F32), g, start, 0) for g in gain_grads
        ]
        gain_grads = [lax.psum_scatter(g, "fsdp", scatter_dimension=0, tiled=True) for g in placed]
    return (query_grad, key_grad, value_grad, *gain_grads)


def solution(mesh):
    placed = (P("ctx", "fsdp"),) * 6 + (P("fsdp"), P("fsdp"), P(), P("ctx"))
    return jax.shard_map(
        per_device,
        mesh=mesh,
        in_specs=placed,
        out_specs=(P("ctx", "fsdp"), P("ctx", "fsdp"), P("ctx", "fsdp"), P("fsdp"), P("fsdp")),
        check_vma=False,
    )
```

```python
import functools
import math

import jax
import jax.numpy as jnp
import numpy as np
from jax import lax
from jax.experimental import pallas as pl
from jax.experimental.pallas import tpu as pltpu
from jax.sharding import PartitionSpec as P


HD = 128
STEPS = 1000

eps_norm = 1e-06
loss_scale = 256.0
rope_base = 10000.0
floor_term = 0.1

BOTH = ("ctx", "fsdp")
F32 = jnp.float32
BF16 = jnp.bfloat16
ORDER_ROWS = 16

NT = (((1,), (1,)), ((), ()))
TN = (((0,), (0,)), ((), ()))
NN = (((1,), (0,)), ((), ()))


def mm(lhs, rhs, dims):
    return lax.dot_general(lhs, rhs, dims, preferred_element_type=F32)


def eye_mask(size):
    rows = lax.broadcasted_iota(jnp.int32, (size, size), 0)
    return rows == lax.broadcasted_iota(jnp.int32, (size, size), 1)


def as_row(column):
    return jnp.sum(jnp.where(eye_mask(column.shape[0]), column, 0.0), axis=0, keepdims=True)


def as_column(row):
    return jnp.sum(jnp.where(eye_mask(row.shape[1]), row, 0.0), axis=1, keepdims=True)


def hosted_head(ctx_id, fsdp_id, n_ctx):
    return (ctx_id + n_ctx - fsdp_id % n_ctx) % n_ctx


def turn(field, cos_t, sin_t):
    return field * cos_t + pltpu.roll(field, HD // 2, 1) * sin_t


def turn_back(field, angles):
    cos_t, sin_t = spread(angles)
    return turn(field, cos_t, -sin_t)


def spread(angles):
    swapped = pltpu.roll(angles, HD // 2, 1)
    low = lax.broadcasted_iota(jnp.int32, angles.shape, 1) < HD // 2
    return jnp.where(low, angles, swapped), jnp.where(low, -swapped, angles)


def head_lanes(head, heads):
    return pl.ds(pl.multiple_of(jnp.minimum(head, heads - 1) * HD, HD), HD)


def norm_scales(stats, channels):
    mean = stats * (1.0 / channels)
    inv = lax.rsqrt(mean[0:2] + eps_norm)
    inv_q, inv_k = as_column(inv[0:1]), as_column(inv[1:2])
    tilt = inv * inv * inv * mean[2:4]
    return inv_q, inv_k, as_column(tilt[0:1]), as_column(tilt[1:2])


def pack_kernel(n_ctx, heads, *refs):
    order_hbm, gain_hbms, field_hbms = refs[0], refs[1:3], refs[3:9]
    stats_ref, gain_refs, block_refs = refs[9], refs[10:12], refs[12 : 12 + n_ctx]
    order_ref, line_refs, field_refs, sems = refs[12 + n_ctx], refs[13 + n_ctx : 15 + n_ctx], refs[15 + n_ctx : -1], refs[-1]
    sources = (*field_hbms, order_hbm, *gain_hbms)
    targets = (*field_refs, order_ref, *line_refs)
    copies = [pltpu.make_async_copy(a, b, sems.at[at]) for at, (a, b) in enumerate(zip(sources, targets))]
    for copy in copies:
        copy.start()
    ctx_id, fsdp_id = lax.axis_index("ctx"), lax.axis_index("fsdp")
    rows = field_refs[0].shape[0]
    for copy in copies:
        copy.wait()
    order = jnp.full((ORDER_ROWS, HD), order_ref[0].astype(F32), F32).astype(BF16)
    for dist, block in enumerate(block_refs):
        lanes = head_lanes(hosted_head(ctx_id ^ dist, fsdp_id, n_ctx), heads)
        for at, ref in enumerate(field_refs):
            block[at * rows : (at + 1) * rows, :] = ref[:, lanes]
        block[6 * rows :, :] = order
    q, k, qt, kt = (field_refs[at][...].astype(F32) for at in (0, 1, 3, 4))
    for at, product in enumerate((q * q, k * k, q * qt, k * kt)):
        stats_ref[at : at + 1, :] = as_row(jnp.sum(product, axis=1, keepdims=True))
    for gain_ref, line_ref in zip(gain_refs, line_refs):
        gain_ref[...] = line_ref[...].reshape(gain_ref.shape)


def forward_kernel(n_ctx, n_fsdp, heads, channels, *refs):
    time_ref, gain_q_ref, gain_k_ref, table_ref = refs[:4]
    block_refs = refs[4 : 4 + n_ctx]
    stats_ref = refs[4 + n_ctx]
    energy_ref, qn_ref, kn_ref, vn_ref, x_ref, goal_ref, lse_ref, drift_ref, turn_ref = refs[5 + n_ctx : -5]
    qcat_ref, kcat_ref, vcat_ref, slots_ref, sem = refs[-5:]
    copy = pltpu.make_async_copy(time_ref, slots_ref, sem)
    copy.start()
    ctx_id, fsdp_id = lax.axis_index("ctx"), lax.axis_index("fsdp")
    head = hosted_head(ctx_id, fsdp_id, n_ctx)
    active = head < heads
    lanes = head_lanes(head, heads)
    gain_q, gain_k = gain_q_ref[:, lanes], gain_k_ref[:, lanes]
    rows = (block_refs[0].shape[0] - ORDER_ROWS) // 6
    inv_root = HD ** (-0.5)
    for dist, block in enumerate(block_refs):
        here = slice(dist * rows, (dist + 1) * rows)
        inv_q, inv_k, tilt_q, tilt_k = norm_scales(stats_ref[4 * dist : 4 * dist + 4, :], channels)
        order = block[6 * rows : 6 * rows + 1, :].astype(F32)
        both = table_ref[0:rows, :]
        for other in range(1, n_ctx):
            both = jnp.where(order == float(other), table_ref[other * rows : (other + 1) * rows, :], both)
        turn_ref[here, :] = both
        cos_t, sin_t = spread(both)

        def part(at):
            return block[at * rows : (at + 1) * rows, :]

        q, k = part(0).astype(F32), part(1).astype(F32)
        qt, kt = part(3).astype(F32), part(4).astype(F32)
        qcat_ref[here, HD:] = turn(q * inv_q * gain_q, cos_t, sin_t).astype(BF16)
        qcat_ref[here, 0:HD] = turn((qt * inv_q - q * tilt_q) * gain_q, cos_t, sin_t).astype(BF16)
        kcat_ref[here, 0:HD] = turn(k * inv_k * gain_k, cos_t, sin_t).astype(BF16)
        kcat_ref[here, HD:] = turn((kt * inv_k - k * tilt_k) * gain_k, cos_t, sin_t).astype(BF16)
        vcat_ref[here, 0:HD] = part(2)
        vcat_ref[here, HD:] = part(5)
        vn_ref[here, :] = part(2)
        x_ref[here, 0:HD] = part(0)
        x_ref[here, HD:] = part(1)
    qn_ref[...] = qcat_ref[:, HD:]
    kn_ref[...] = kcat_ref[:, 0:HD]
    copy.wait()
    picked = slots_ref[fsdp_id // (channels // (heads * HD))].astype(F32)
    angle_t = jnp.full((8, HD), 0.5 * math.pi * (picked + 0.5) / STEPS)
    coef_out = (jnp.sin(angle_t) * jnp.cos(angle_t))[0:1]
    coef_tan = (jnp.cos(angle_t) ** 2)[0:1]
    for dist in range(n_ctx):
        here = slice(dist * rows, (dist + 1) * rows)
        scores = mm(qcat_ref[here, HD:], kcat_ref[:, 0:HD], NT) * inv_root
        slopes = mm(qcat_ref[here, :], kcat_ref[...], NT) * inv_root
        peak = jnp.max(scores, axis=1, keepdims=True)
        weights = jnp.exp(scores - peak)
        totals = jnp.sum(weights, axis=1, keepdims=True)
        tilted = weights * slopes
        numer = mm(weights.astype(BF16), vcat_ref[...], NN)
        numer_tan = numer[:, HD:] + mm(tilted.astype(BF16), vcat_ref[:, 0:HD], NN)
        tilt = jnp.sum(tilted, axis=1, keepdims=True)
        output = numer[:, 0:HD] / totals
        output_tan = numer_tan / totals - (tilt / totals) * output
        goal = coef_out * output + coef_tan * output_tan
        goal_ref[here, :] = goal
        drift_ref[:, here] = as_row(
            jnp.sum(goal.astype(BF16).astype(F32) * output, axis=1, keepdims=True)
        )
        lse_ref[:, here] = as_row(peak + jnp.log(totals))
        row = as_row(jnp.sum(goal * goal, axis=1, keepdims=True))
        energy_ref[0, pl.ds(ctx_id ^ dist, 1), :] = jnp.where(active, row, 0.0)
    first = energy_ref[0]
    for at in range(1, energy_ref.shape[0]):
        energy_ref[at] = first


def token_levels(energy_ref, n_ctx, n_fsdp, head_split, channels):
    sample = lax.axis_index("fsdp") // head_split
    energy = sum(
        jnp.sum(energy_ref[pl.ds(at * n_fsdp + sample * head_split, head_split)], axis=0)
        for at in range(n_ctx)
    )
    return loss_scale / (jnp.sqrt(energy * (1.0 / channels)) + floor_term)


def pick_row(table, at):
    ids = lax.broadcasted_iota(jnp.int32, table.shape, 0)
    return jnp.sum(jnp.where(ids == at, table, 0.0), axis=0, keepdims=True)


def query_kernel(n_ctx, heads, channels, *refs):
    gain_ref, qn_ref, kn_ref, vn_ref, x_ref, goal_ref, lse_ref, drift_ref, turn_ref, stats_ref = refs[:10]
    probs_ref, dscore_ref, cross_ref, lift_ref, grown_ref, goal_b_ref, dscore_b_ref = refs[10:]
    head = hosted_head(lax.axis_index("ctx"), lax.axis_index("fsdp"), n_ctx)
    gain = gain_ref[:, head_lanes(head, heads)]
    rows = cross_ref.shape[1]
    inv_root = HD ** (-0.5)
    goal_b_ref[...] = goal_ref[...].astype(BF16)
    blocks = [slice(dist * rows, (dist + 1) * rows) for dist in range(n_ctx)]
    for here in blocks:
        scores = mm(kn_ref[here, :], qn_ref[...], NT) * inv_root
        probs = jnp.exp(scores - lse_ref[...])
        dprobs = mm(vn_ref[here, :], goal_b_ref[...], NT)
        dscore = probs * (dprobs - drift_ref[...]) * inv_root
        probs_ref[here, :] = probs.astype(BF16)
        dscore_ref[here, :] = dscore
        dscore_b_ref[here, :] = dscore.astype(BF16)
    for dist, here in enumerate(blocks):
        dquery = mm(dscore_b_ref[:, here], kn_ref[...], TN)
        inv_q = norm_scales(stats_ref[4 * dist : 4 * dist + 4, :], channels)[0]
        x = x_ref[here, 0:HD].astype(F32)
        dy = turn_back(dquery, turn_ref[here, :])
        grown = gain * dy
        grown_ref[here, :] = grown
        cross_ref[dist : dist + 1, :] = as_row(jnp.sum(x * grown, axis=1, keepdims=True))
        lift_ref[here, :] = dy * x * inv_q


def key_kernel(n_ctx, n_fsdp, heads, channels, *refs):
    energy_ref, gain_ref, qn_ref, x_ref, goal_ref, turn_ref, stats_ref = refs[:7]
    probs_ref, dscore_ref, cross_q_ref, lift_ref, grown_ref, cross_ref = refs[7:13]
    back_refs = refs[13 : 13 + n_ctx]
    cot_ref = refs[13 + n_ctx]
    ctx_id, fsdp_id = lax.axis_index("ctx"), lax.axis_index("fsdp")
    head = hosted_head(ctx_id, fsdp_id, n_ctx)
    active = head < heads
    gain = gain_ref[:, head_lanes(head, heads)]
    rows = cross_q_ref.shape[1]
    level = token_levels(energy_ref, n_ctx, n_fsdp, channels // (heads * HD), channels)
    levels = [pick_row(level, ctx_id ^ dist) for dist in range(n_ctx)]
    blocks = [slice(dist * rows, (dist + 1) * rows) for dist in range(n_ctx)]
    gain_q_sum = jnp.zeros((1, HD), F32)
    for here, row, back in zip(blocks, levels, back_refs):
        scale = as_column(row)
        back[0:rows, :] = (scale * grown_ref[here, :]).astype(BF16)
        cot_ref[here, :] = (scale * goal_ref[here, :]).astype(BF16)
        gain_q_sum = gain_q_sum + jnp.sum(scale * lift_ref[here, :], axis=0, keepdims=True)
    level_row = jnp.concatenate(levels, axis=1)
    gain_k_sum = jnp.zeros((1, HD), F32)
    cross_k = []
    for dist, here in enumerate(blocks):
        back_refs[dist][2 * rows :, :] = mm(probs_ref[here, :], cot_ref[...], NN).astype(BF16)
        dscore = (dscore_ref[here, :] * level_row).astype(BF16)
        dkey = mm(dscore, qn_ref[...], NN)
        inv_k = norm_scales(stats_ref[4 * dist : 4 * dist + 4, :], channels)[1]
        x = x_ref[here, HD:].astype(F32)
        dy = turn_back(dkey, turn_ref[here, :])
        grown = gain * dy
        back_refs[dist][rows : 2 * rows, :] = grown.astype(BF16)
        cross_k.append(as_row(jnp.sum(x * grown, axis=1, keepdims=True)))
        gain_k_sum = gain_k_sum + jnp.sum(dy * x * inv_k, axis=0, keepdims=True)
    for dist in range(n_ctx):
        cross_q = cross_q_ref[dist : dist + 1, :] * levels[dist]
        sums = jnp.concatenate([cross_q, cross_k[dist], gain_q_sum, gain_k_sum], axis=0)
        sums = jnp.where(active, sums, 0.0)
        start = (ctx_id ^ dist) * n_fsdp
        for at in range(n_fsdp):
            cross_ref[start + at] = sums


def finish_kernel(n_ctx, n_fsdp, heads, channels, *refs):
    stats_ref, cross_ref, q_ref, k_ref = refs[:4]
    back_refs = refs[4 : 4 + n_ctx]
    dq_ref, dk_ref, dv_ref, dgain_q_ref, dgain_k_ref, gain_q_ref, gain_k_ref = refs[4 + n_ctx :]
    ctx_id, fsdp_id = lax.axis_index("ctx"), lax.axis_index("fsdp")
    head_split = channels // (heads * HD)
    sample = fsdp_id // head_split
    rows = q_ref.shape[0]
    inv_q, inv_k, _, _ = norm_scales(stats_ref[0:4, :], channels)
    total = jnp.zeros((4, rows), F32)
    for ctx_at in range(n_ctx):
        total = total + jnp.sum(cross_ref[pl.ds(ctx_at * n_fsdp + sample * head_split, head_split)], axis=0)
    mean = total[0:2] * (1.0 / channels)
    tilt_q = inv_q * inv_q * inv_q * as_column(mean[0:1])
    tilt_k = inv_k * inv_k * inv_k * as_column(mean[1:2])
    for dist in range(n_ctx):
        host = ctx_id ^ dist
        head = hosted_head(host, fsdp_id, n_ctx)

        @pl.when(head < heads)
        def _(dist=dist, host=host, head=head):
            back = back_refs[dist]
            lanes = head_lanes(head, heads)
            h_q, h_k = back[0:rows, :].astype(F32), back[rows : 2 * rows, :].astype(F32)
            dq_ref[:, lanes] = (inv_q * h_q - q_ref[:, lanes].astype(F32) * tilt_q).astype(BF16)
            dk_ref[:, lanes] = (inv_k * h_k - k_ref[:, lanes].astype(F32) * tilt_k).astype(BF16)
            dv_ref[:, lanes] = back[2 * rows :, :]
            sums = cross_ref[host * n_fsdp + fsdp_id]
            gain_q_ref[:, lanes] = sums[2:3]
            gain_k_ref[:, lanes] = sums[3:4]

    dgain_q_ref[...] = gain_q_ref[...].reshape(dgain_q_ref.shape)
    dgain_k_ref[...] = gain_k_ref[...].reshape(dgain_k_ref.shape)


def per_device(
    queries,
    keys,
    values,
    query_tangent,
    key_tangent,
    value_tangent,
    query_gain,
    key_gain,
    time_index,
    shard_order,
):
    n_ctx, n_fsdp = lax.axis_size("ctx"), lax.axis_size("fsdp")
    n_all = n_ctx * n_fsdp
    fsdp_id = lax.axis_index("fsdp")
    rows, ch_dev = queries.shape
    heads = ch_dev // HD
    channels = query_gain.shape[0] * n_fsdp
    head_split = channels // ch_dev
    seq = rows * n_ctx
    sizes = (n_ctx, n_fsdp, heads, channels)

    vmem = pl.BlockSpec(memory_space=pltpu.VMEM)

    hbm = pl.BlockSpec(memory_space=pltpu.HBM)

    def kernel(body, ins, outs, scratch=(), flops=10**8, from_hbm=0):
        return pl.pallas_call(
            body,
            out_shape=[jax.ShapeDtypeStruct(*o) for o in outs],
            in_specs=[hbm] * from_hbm + [vmem] * (len(ins) - from_hbm),
            out_specs=[vmem] * len(outs),
            scratch_shapes=list(scratch),
            cost_estimate=pl.CostEstimate(flops=flops, bytes_accessed=2**20, transcendentals=0),
            compiler_params=pltpu.CompilerParams(vmem_limit_bytes=16 * 2**20 + seq * 2**14),
        )(*ins)

    def in_hbm(array):
        return pltpu.with_memory_space_constraint(array, pltpu.HBM)

    def swap(block, axis, dist):
        return lax.ppermute(block, axis, [(i, i ^ dist) for i in range(lax.axis_size(axis))])

    def sum_over_sample(block):
        block = block + swap(block, "fsdp", 1)
        return sum([swap(block, "fsdp", d) for d in range(2, head_split, 2)], block)

    def from_peers(blocks, idle=None):
        out = [blocks[0]] + [None] * (n_ctx - 1)
        for dist in reversed(range(1, n_ctx)):
            route = []
            for c in range(n_ctx):
                for f in range(n_fsdp):
                    near = idle and idle(c, c ^ dist, f) and idle(c ^ dist, c, f ^ 1)
                    target = (c, f ^ 1) if near else (c ^ dist, f)
                    route.append((c * n_fsdp + f, target[0] * n_fsdp + target[1]))
            out[dist] = lax.ppermute(blocks[dist], BOTH, route)
        return out

    places = np.arange(seq, dtype=np.float32)
    freqs = (rope_base ** (-np.arange(HD // 2) / (HD // 2))).astype(np.float32)
    angles = (places[:, None] * freqs[None, :]).astype(np.float64)
    table = jnp.asarray(np.concatenate([np.cos(angles), np.sin(angles)], axis=1).astype(np.float32))

    gains = (query_gain, key_gain)
    if query_gain.shape[0] != ch_dev:
        start = (fsdp_id % head_split) * ch_dev
        gains = [lax.all_gather(g, "fsdp", axis=0, tiled=True) for g in gains]
        gains = [lax.dynamic_slice_in_dim(g, start, ch_dev, 0) for g in gains]

    fields = (queries, keys, values, query_tangent, key_tangent, value_tangent)
    gains = [in_hbm(a) for a in gains]
    fields = [in_hbm(a) for a in fields]
    part, gain_q, gain_k, *blocks = kernel(
        functools.partial(pack_kernel, n_ctx, heads),
        (shard_order, *gains, *fields),
        [((4, rows), F32)] + [((1, ch_dev), F32)] * 2 + [((6 * rows + ORDER_ROWS, HD), BF16)] * n_ctx,
        scratch=[pltpu.SMEM((1,), jnp.int32)]
        + [pltpu.VMEM((ch_dev,), F32)] * 2
        + [pltpu.VMEM((rows, ch_dev), BF16)] * 6
        + [pltpu.SemaphoreType.DMA((9,))],
        from_hbm=9,
    )
    gains = (gain_q, gain_k)
    parts = from_peers([part] * n_ctx)
    blocks = from_peers(blocks, lambda c, peer, f: hosted_head(peer, f, n_ctx) >= heads)
    stats = sum_over_sample(jnp.concatenate(parts, axis=0))

    energy_out, qn, kn, vn, x, goal, lse, drift, turns = kernel(
        functools.partial(forward_kernel, *sizes),
        (time_index, *gains, table, *blocks, stats),
        [((n_all, n_ctx, rows), F32)]
        + [((seq, HD), BF16)] * 3
        + [((seq, 2 * HD), BF16), ((seq, HD), F32)]
        + [((1, seq), F32)] * 2
        + [((seq, HD), F32)],
        scratch=[pltpu.VMEM((seq, 2 * HD), BF16)] * 3
        + [pltpu.SMEM(time_index.shape, jnp.int32), pltpu.SemaphoreType.DMA],
        from_hbm=1,
    )
    energy = lax.all_to_all(energy_out, BOTH, 0, 0)
    probs, dscore, cross_q, lift, grown = kernel(
        functools.partial(query_kernel, n_ctx, heads, channels),
        (gain_q, qn, kn, vn, x, goal, lse, drift, turns, stats),
        [((seq, seq), BF16), ((seq, seq), F32), ((n_ctx, rows), F32)] + [((seq, HD), F32)] * 2,
        scratch=[pltpu.VMEM((seq, HD), BF16), pltpu.VMEM((seq, seq), BF16)],
    )

    cross_out, *back = kernel(
        functools.partial(key_kernel, *sizes),
        (energy, gain_k, qn, x, goal, turns, stats, probs, dscore, cross_q, lift, grown),
        [((n_all, 4, rows), F32)] + [((3 * rows, HD), BF16)] * n_ctx,
        scratch=[pltpu.VMEM((seq, HD), BF16)],
    )
    back = from_peers(back, lambda c, peer, f: hosted_head(c, f, n_ctx) >= heads)
    crosses = lax.all_to_all(cross_out, BOTH, 0, 0)

    query_grad, key_grad, value_grad, *gain_grads = kernel(
        functools.partial(finish_kernel, *sizes),
        (stats, crosses, queries, keys, *back),
        [((rows, ch_dev), BF16)] * 3 + [((ch_dev,), F32)] * 2,
        scratch=[pltpu.VMEM((1, ch_dev), F32)] * 2,
    )
    if query_gain.shape[0] != ch_dev:
        placed = [
            lax.dynamic_update_slice_in_dim(jnp.zeros((channels,), F32), g, start, 0) for g in gain_grads
        ]
        gain_grads = [lax.psum_scatter(g, "fsdp", scatter_dimension=0, tiled=True) for g in placed]
    return (query_grad, key_grad, value_grad, *gain_grads)


def solution(mesh):
    placed = (P("ctx", "fsdp"),) * 6 + (P("fsdp"), P("fsdp"), P(), P("ctx"))
    return jax.shard_map(
        per_device,
        mesh=mesh,
        in_specs=placed,
        out_specs=(P("ctx", "fsdp"), P("ctx", "fsdp"), P("ctx", "fsdp"), P("fsdp"), P("fsdp")),
        check_vma=False,
    )
```

```python
import functools
import math

import jax
import jax.numpy as jnp
import numpy as np
from jax import lax
from jax.experimental import pallas as pl
from jax.experimental.pallas import tpu as pltpu
from jax.sharding import PartitionSpec as P


HD = 128
STEPS = 1000

eps_norm = 1e-06
loss_scale = 256.0
rope_base = 10000.0
floor_term = 0.1

BOTH = ("ctx", "fsdp")
F32 = jnp.float32
BF16 = jnp.bfloat16
ORDER_ROWS = 16

NT = (((1,), (1,)), ((), ()))
TN = (((0,), (0,)), ((), ()))
NN = (((1,), (0,)), ((), ()))


def mm(lhs, rhs, dims):
    return lax.dot_general(lhs, rhs, dims, preferred_element_type=F32)


def eye_mask(size):
    rows = lax.broadcasted_iota(jnp.int32, (size, size), 0)
    return rows == lax.broadcasted_iota(jnp.int32, (size, size), 1)


def as_row(column):
    return jnp.sum(jnp.where(eye_mask(column.shape[0]), column, 0.0), axis=0, keepdims=True)


def columns(rows):
    mask = eye_mask(rows.shape[1])
    return [
        jnp.sum(jnp.where(mask, rows[at : at + 1], 0.0), axis=1, keepdims=True)
        for at in range(rows.shape[0])
    ]


def hosted_head(ctx_id, fsdp_id, n_ctx):
    return (ctx_id + n_ctx - fsdp_id % n_ctx) % n_ctx


def turn(field, cos_t, sin_t):
    return field * cos_t + pltpu.roll(field, HD // 2, 1) * sin_t


def turn_back(field, angles):
    cos_t, sin_t = spread(angles)
    return turn(field, cos_t, -sin_t)


def spread(angles):
    swapped = pltpu.roll(angles, HD // 2, 1)
    low = lax.broadcasted_iota(jnp.int32, angles.shape, 1) < HD // 2
    return jnp.where(low, angles, swapped), jnp.where(low, -swapped, angles)


def head_lanes(head, heads):
    return pl.ds(pl.multiple_of(jnp.minimum(head, heads - 1) * HD, HD), HD)


def norm_scales(stats, channels):
    return lax.rsqrt(stats[0:2] * (1.0 / channels) + eps_norm)


def norm_columns(stats, channels):
    inv = norm_scales(stats, channels)
    tilt = inv * inv * inv * (stats[2:4] * (1.0 / channels))
    return columns(jnp.concatenate([inv, tilt], axis=0))


def pack_kernel(n_ctx, heads, *refs):
    order_hbm, gain_hbms, field_hbms = refs[0], refs[1:3], refs[3:9]
    stats_ref, gain_refs, block_refs = refs[9], refs[10:12], refs[12 : 12 + n_ctx]
    order_ref, line_refs, field_refs, sems = refs[12 + n_ctx], refs[13 + n_ctx : 15 + n_ctx], refs[15 + n_ctx : -1], refs[-1]
    sources = (*field_hbms, order_hbm, *gain_hbms)
    targets = (*field_refs, order_ref, *line_refs)
    copies = [pltpu.make_async_copy(a, b, sems.at[at]) for at, (a, b) in enumerate(zip(sources, targets))]
    for copy in copies:
        copy.start()
    ctx_id, fsdp_id = lax.axis_index("ctx"), lax.axis_index("fsdp")
    rows = field_refs[0].shape[0]
    for copy in copies:
        copy.wait()
    order = jnp.full((ORDER_ROWS, HD), order_ref[0].astype(F32), F32).astype(BF16)
    for dist, block in enumerate(block_refs):
        lanes = head_lanes(hosted_head(ctx_id ^ dist, fsdp_id, n_ctx), heads)
        for at, ref in enumerate(field_refs):
            block[at * rows : (at + 1) * rows, :] = ref[:, lanes]
        block[6 * rows :, :] = order
    q, k, qt, kt = (field_refs[at][...].astype(F32) for at in (0, 1, 3, 4))
    for at, product in enumerate((q * q, k * k, q * qt, k * kt)):
        stats_ref[at : at + 1, :] = as_row(jnp.sum(product, axis=1, keepdims=True))
    for gain_ref, line_ref in zip(gain_refs, line_refs):
        gain_ref[...] = line_ref[...].reshape(gain_ref.shape)


def forward_kernel(n_ctx, n_fsdp, heads, channels, *refs):
    time_ref, gain_q_ref, gain_k_ref, table_ref = refs[:4]
    block_refs = refs[4 : 4 + n_ctx]
    stats_ref = refs[4 + n_ctx]
    energy_ref, qn_ref, kn_ref, vn_ref, x_ref, goal_ref, lse_ref, drift_ref, turn_ref = refs[5 + n_ctx : -5]
    qcat_ref, kcat_ref, vcat_ref, slots_ref, sem = refs[-5:]
    copy = pltpu.make_async_copy(time_ref, slots_ref, sem)
    copy.start()
    ctx_id, fsdp_id = lax.axis_index("ctx"), lax.axis_index("fsdp")
    head = hosted_head(ctx_id, fsdp_id, n_ctx)
    active = head < heads
    lanes = head_lanes(head, heads)
    gain_q, gain_k = gain_q_ref[:, lanes], gain_k_ref[:, lanes]
    rows = (block_refs[0].shape[0] - ORDER_ROWS) // 6
    inv_root = HD ** (-0.5)
    for dist, block in enumerate(block_refs):
        here = slice(dist * rows, (dist + 1) * rows)
        inv_q, inv_k, tilt_q, tilt_k = norm_columns(stats_ref[4 * dist : 4 * dist + 4, :], channels)
        order = block[6 * rows : 6 * rows + 1, :].astype(F32)
        both = table_ref[0:rows, :]
        for other in range(1, n_ctx):
            both = jnp.where(order == float(other), table_ref[other * rows : (other + 1) * rows, :], both)
        turn_ref[here, :] = both
        cos_t, sin_t = spread(both)

        def part(at):
            return block[at * rows : (at + 1) * rows, :]

        q, k = part(0).astype(F32), part(1).astype(F32)
        qt, kt = part(3).astype(F32), part(4).astype(F32)
        qcat_ref[here, HD:] = turn(q * inv_q * gain_q, cos_t, sin_t).astype(BF16)
        qcat_ref[here, 0:HD] = turn((qt * inv_q - q * tilt_q) * gain_q, cos_t, sin_t).astype(BF16)
        kcat_ref[here, 0:HD] = turn(k * inv_k * gain_k, cos_t, sin_t).astype(BF16)
        kcat_ref[here, HD:] = turn((kt * inv_k - k * tilt_k) * gain_k, cos_t, sin_t).astype(BF16)
        vcat_ref[here, 0:HD] = part(2)
        vcat_ref[here, HD:] = part(5)
        vn_ref[here, :] = part(2)
        x_ref[here, 0:HD] = part(0)
        x_ref[here, HD:] = part(1)
    qn_ref[...] = qcat_ref[:, HD:]
    kn_ref[...] = kcat_ref[:, 0:HD]
    copy.wait()
    picked = slots_ref[fsdp_id // (channels // (heads * HD))].astype(F32)
    angle_t = jnp.full((8, HD), 0.5 * math.pi * (picked + 0.5) / STEPS)
    coef_out = (jnp.sin(angle_t) * jnp.cos(angle_t))[0:1]
    coef_tan = (jnp.cos(angle_t) ** 2)[0:1]
    for dist in range(n_ctx):
        here = slice(dist * rows, (dist + 1) * rows)
        scores = mm(qcat_ref[here, HD:], kcat_ref[:, 0:HD], NT)
        slopes = mm(qcat_ref[here, :], kcat_ref[...], NT)
        peak = jnp.max(scores, axis=1, keepdims=True)
        weights = jnp.exp((scores - peak) * inv_root)
        totals = jnp.sum(weights, axis=1, keepdims=True)
        tilted = weights * slopes
        numer = mm(weights.astype(BF16), vcat_ref[...], NN)
        numer_tan = numer[:, HD:] + inv_root * mm(tilted.astype(BF16), vcat_ref[:, 0:HD], NN)
        tilt = jnp.sum(tilted, axis=1, keepdims=True) * inv_root
        output = numer[:, 0:HD] / totals
        output_tan = (numer_tan - tilt * output) / totals
        goal = coef_out * output + coef_tan * output_tan
        goal_ref[here, :] = goal
        drift_ref[:, here] = as_row(
            jnp.sum(goal.astype(BF16).astype(F32) * output, axis=1, keepdims=True)
        )
        lse_ref[:, here] = as_row(peak * inv_root + jnp.log(totals))
        row = as_row(jnp.sum(goal * goal, axis=1, keepdims=True))
        energy_ref[0, pl.ds(ctx_id ^ dist, 1), :] = jnp.where(active, row, 0.0)
    first = energy_ref[0]
    for at in range(1, energy_ref.shape[0]):
        energy_ref[at] = first


def token_levels(energy_ref, n_ctx, n_fsdp, head_split, channels):
    sample = lax.axis_index("fsdp") // head_split
    energy = sum(
        jnp.sum(energy_ref[pl.ds(at * n_fsdp + sample * head_split, head_split)], axis=0)
        for at in range(n_ctx)
    )
    return loss_scale / (jnp.sqrt(energy * (1.0 / channels)) + floor_term)


def pick_row(table, at):
    ids = lax.broadcasted_iota(jnp.int32, table.shape, 0)
    return jnp.sum(jnp.where(ids == at, table, 0.0), axis=0, keepdims=True)


def query_kernel(n_ctx, heads, channels, *refs):
    gain_ref, qn_ref, kn_ref, vn_ref, x_ref, goal_ref, lse_ref, drift_ref, turn_ref, stats_ref = refs[:10]
    probs_ref, dscore_ref, cross_ref, lift_ref, grown_ref, goal_b_ref, dscore_b_ref = refs[10:]
    head = hosted_head(lax.axis_index("ctx"), lax.axis_index("fsdp"), n_ctx)
    gain = gain_ref[:, head_lanes(head, heads)]
    rows = cross_ref.shape[1]
    inv_root = HD ** (-0.5)
    goal_b_ref[...] = goal_ref[...].astype(BF16)
    blocks = [slice(dist * rows, (dist + 1) * rows) for dist in range(n_ctx)]
    for here in blocks:
        scores = mm(kn_ref[here, :], qn_ref[...], NT)
        probs = jnp.exp(scores * inv_root - lse_ref[...])
        dprobs = mm(vn_ref[here, :], goal_b_ref[...], NT)
        dscore = probs * (dprobs - drift_ref[...])
        probs_ref[here, :] = probs.astype(BF16)
        dscore_ref[here, :] = dscore
        dscore_b_ref[here, :] = dscore.astype(BF16)
    for dist, here in enumerate(blocks):
        dquery = mm(dscore_b_ref[:, here], kn_ref[...], TN) * inv_root
        (inv_q,) = columns(norm_scales(stats_ref[4 * dist : 4 * dist + 4, :], channels)[0:1])
        x = x_ref[here, 0:HD].astype(F32)
        dy = turn_back(dquery, turn_ref[here, :])
        grown = gain * dy
        grown_ref[here, :] = grown
        cross_ref[dist : dist + 1, :] = as_row(jnp.sum(x * grown, axis=1, keepdims=True))
        lift_ref[here, :] = dy * x * inv_q


def key_kernel(n_ctx, n_fsdp, heads, channels, *refs):
    energy_ref, gain_ref, qn_ref, x_ref, goal_ref, turn_ref, stats_ref = refs[:7]
    probs_ref, dscore_ref, cross_q_ref, lift_ref, grown_ref, cross_ref = refs[7:13]
    back_refs = refs[13 : 13 + n_ctx]
    cot_ref = refs[13 + n_ctx]
    ctx_id, fsdp_id = lax.axis_index("ctx"), lax.axis_index("fsdp")
    head = hosted_head(ctx_id, fsdp_id, n_ctx)
    active = head < heads
    gain = gain_ref[:, head_lanes(head, heads)]
    rows = cross_q_ref.shape[1]
    level = token_levels(energy_ref, n_ctx, n_fsdp, channels // (heads * HD), channels)
    levels = [pick_row(level, ctx_id ^ dist) for dist in range(n_ctx)]
    blocks = [slice(dist * rows, (dist + 1) * rows) for dist in range(n_ctx)]
    gain_q_sum = jnp.zeros((1, HD), F32)
    for here, row, back in zip(blocks, levels, back_refs):
        (scale,) = columns(row)
        back[0:rows, :] = (scale * grown_ref[here, :]).astype(BF16)
        cot_ref[here, :] = (scale * goal_ref[here, :]).astype(BF16)
        gain_q_sum = gain_q_sum + jnp.sum(scale * lift_ref[here, :], axis=0, keepdims=True)
    level_row = jnp.concatenate(levels, axis=1) * HD ** (-0.5)
    gain_k_sum = jnp.zeros((1, HD), F32)
    cross_k = []
    for dist, here in enumerate(blocks):
        back_refs[dist][2 * rows :, :] = mm(probs_ref[here, :], cot_ref[...], NN).astype(BF16)
        dscore = (dscore_ref[here, :] * level_row).astype(BF16)
        dkey = mm(dscore, qn_ref[...], NN)
        (inv_k,) = columns(norm_scales(stats_ref[4 * dist : 4 * dist + 4, :], channels)[1:2])
        x = x_ref[here, HD:].astype(F32)
        dy = turn_back(dkey, turn_ref[here, :])
        grown = gain * dy
        back_refs[dist][rows : 2 * rows, :] = grown.astype(BF16)
        cross_k.append(as_row(jnp.sum(x * grown, axis=1, keepdims=True)))
        gain_k_sum = gain_k_sum + jnp.sum(dy * x * inv_k, axis=0, keepdims=True)
    for dist in range(n_ctx):
        cross_q = cross_q_ref[dist : dist + 1, :] * levels[dist]
        sums = jnp.concatenate([cross_q, cross_k[dist], gain_q_sum, gain_k_sum], axis=0)
        sums = jnp.where(active, sums, 0.0)
        start = (ctx_id ^ dist) * n_fsdp
        for at in range(n_fsdp):
            cross_ref[start + at] = sums


def finish_kernel(n_ctx, n_fsdp, heads, channels, *refs):
    stats_ref, cross_ref, q_ref, k_ref = refs[:4]
    back_refs = refs[4 : 4 + n_ctx]
    dq_ref, dk_ref, dv_ref, dgain_q_ref, dgain_k_ref, gain_q_ref, gain_k_ref = refs[4 + n_ctx :]
    ctx_id, fsdp_id = lax.axis_index("ctx"), lax.axis_index("fsdp")
    head_split = channels // (heads * HD)
    sample = fsdp_id // head_split
    rows = q_ref.shape[0]
    inv = norm_scales(stats_ref[0:4, :], channels)
    total = jnp.zeros((4, rows), F32)
    for ctx_at in range(n_ctx):
        total = total + jnp.sum(cross_ref[pl.ds(ctx_at * n_fsdp + sample * head_split, head_split)], axis=0)
    tilt = inv * inv * inv * (total[0:2] * (1.0 / channels))
    inv_q, inv_k, tilt_q, tilt_k = columns(jnp.concatenate([inv, tilt], axis=0))
    for dist in range(n_ctx):
        host = ctx_id ^ dist
        head = hosted_head(host, fsdp_id, n_ctx)

        @pl.when(head < heads)
        def _(dist=dist, host=host, head=head):
            back = back_refs[dist]
            lanes = head_lanes(head, heads)
            h_q, h_k = back[0:rows, :].astype(F32), back[rows : 2 * rows, :].astype(F32)
            dq_ref[:, lanes] = (inv_q * h_q - q_ref[:, lanes].astype(F32) * tilt_q).astype(BF16)
            dk_ref[:, lanes] = (inv_k * h_k - k_ref[:, lanes].astype(F32) * tilt_k).astype(BF16)
            dv_ref[:, lanes] = back[2 * rows :, :]
            sums = cross_ref[host * n_fsdp + fsdp_id]
            gain_q_ref[:, lanes] = sums[2:3]
            gain_k_ref[:, lanes] = sums[3:4]

    dgain_q_ref[...] = gain_q_ref[...].reshape(dgain_q_ref.shape)
    dgain_k_ref[...] = gain_k_ref[...].reshape(dgain_k_ref.shape)


def per_device(
    queries,
    keys,
    values,
    query_tangent,
    key_tangent,
    value_tangent,
    query_gain,
    key_gain,
    time_index,
    shard_order,
):
    n_ctx, n_fsdp = lax.axis_size("ctx"), lax.axis_size("fsdp")
    n_all = n_ctx * n_fsdp
    fsdp_id = lax.axis_index("fsdp")
    rows, ch_dev = queries.shape
    heads = ch_dev // HD
    channels = query_gain.shape[0] * n_fsdp
    head_split = channels // ch_dev
    seq = rows * n_ctx
    sizes = (n_ctx, n_fsdp, heads, channels)

    vmem = pl.BlockSpec(memory_space=pltpu.VMEM)

    hbm = pl.BlockSpec(memory_space=pltpu.HBM)

    def kernel(body, ins, outs, scratch=(), flops=10**8, from_hbm=0):
        return pl.pallas_call(
            body,
            out_shape=[jax.ShapeDtypeStruct(*o) for o in outs],
            in_specs=[hbm] * from_hbm + [vmem] * (len(ins) - from_hbm),
            out_specs=[vmem] * len(outs),
            scratch_shapes=list(scratch),
            cost_estimate=pl.CostEstimate(flops=flops, bytes_accessed=2**20, transcendentals=0),
            compiler_params=pltpu.CompilerParams(vmem_limit_bytes=16 * 2**20 + seq * 2**14),
        )(*ins)

    def in_hbm(array):
        return pltpu.with_memory_space_constraint(array, pltpu.HBM)

    def swap(block, axis, dist):
        return lax.ppermute(block, axis, [(i, i ^ dist) for i in range(lax.axis_size(axis))])

    def sum_over_sample(block):
        block = block + swap(block, "fsdp", 1)
        return sum([swap(block, "fsdp", d) for d in range(2, head_split, 2)], block)

    def from_peers(blocks, idle=None):
        out = [blocks[0]] + [None] * (n_ctx - 1)
        for dist in reversed(range(1, n_ctx)):
            route = []
            for c in range(n_ctx):
                for f in range(n_fsdp):
                    near = idle and idle(c, c ^ dist, f) and idle(c ^ dist, c, f ^ 1)
                    target = (c, f ^ 1) if near else (c ^ dist, f)
                    route.append((c * n_fsdp + f, target[0] * n_fsdp + target[1]))
            out[dist] = lax.ppermute(blocks[dist], BOTH, route)
        return out

    places = np.arange(seq, dtype=np.float32)
    freqs = (rope_base ** (-np.arange(HD // 2) / (HD // 2))).astype(np.float32)
    angles = (places[:, None] * freqs[None, :]).astype(np.float64)
    table = jnp.asarray(np.concatenate([np.cos(angles), np.sin(angles)], axis=1).astype(np.float32))

    gains = (query_gain, key_gain)
    if query_gain.shape[0] != ch_dev:
        start = (fsdp_id % head_split) * ch_dev
        gains = [lax.all_gather(g, "fsdp", axis=0, tiled=True) for g in gains]
        gains = [lax.dynamic_slice_in_dim(g, start, ch_dev, 0) for g in gains]

    fields = (queries, keys, values, query_tangent, key_tangent, value_tangent)
    gains = [in_hbm(a) for a in gains]
    fields = [in_hbm(a) for a in fields]
    part, gain_q, gain_k, *blocks = kernel(
        functools.partial(pack_kernel, n_ctx, heads),
        (shard_order, *gains, *fields),
        [((4, rows), F32)] + [((1, ch_dev), F32)] * 2 + [((6 * rows + ORDER_ROWS, HD), BF16)] * n_ctx,
        scratch=[pltpu.SMEM((1,), jnp.int32)]
        + [pltpu.VMEM((ch_dev,), F32)] * 2
        + [pltpu.VMEM((rows, ch_dev), BF16)] * 6
        + [pltpu.SemaphoreType.DMA((9,))],
        from_hbm=9,
    )
    gains = (gain_q, gain_k)
    parts = from_peers([part] * n_ctx)
    blocks = from_peers(blocks, lambda c, peer, f: hosted_head(peer, f, n_ctx) >= heads)
    stats = sum_over_sample(jnp.concatenate(parts, axis=0))

    energy_out, qn, kn, vn, x, goal, lse, drift, turns = kernel(
        functools.partial(forward_kernel, *sizes),
        (time_index, *gains, table, *blocks, stats),
        [((n_all, n_ctx, rows), F32)]
        + [((seq, HD), BF16)] * 3
        + [((seq, 2 * HD), BF16), ((seq, HD), F32)]
        + [((1, seq), F32)] * 2
        + [((seq, HD), F32)],
        scratch=[pltpu.VMEM((seq, 2 * HD), BF16)] * 3
        + [pltpu.SMEM(time_index.shape, jnp.int32), pltpu.SemaphoreType.DMA],
        from_hbm=1,
    )
    energy = lax.all_to_all(energy_out, BOTH, 0, 0)
    probs, dscore, cross_q, lift, grown = kernel(
        functools.partial(query_kernel, n_ctx, heads, channels),
        (gain_q, qn, kn, vn, x, goal, lse, drift, turns, stats),
        [((seq, seq), BF16), ((seq, seq), F32), ((n_ctx, rows), F32)] + [((seq, HD), F32)] * 2,
        scratch=[pltpu.VMEM((seq, HD), BF16), pltpu.VMEM((seq, seq), BF16)],
    )

    cross_out, *back = kernel(
        functools.partial(key_kernel, *sizes),
        (energy, gain_k, qn, x, goal, turns, stats, probs, dscore, cross_q, lift, grown),
        [((n_all, 4, rows), F32)] + [((3 * rows, HD), BF16)] * n_ctx,
        scratch=[pltpu.VMEM((seq, HD), BF16)],
    )
    back = from_peers(back, lambda c, peer, f: hosted_head(c, f, n_ctx) >= heads)
    crosses = lax.all_to_all(cross_out, BOTH, 0, 0)

    query_grad, key_grad, value_grad, *gain_grads = kernel(
        functools.partial(finish_kernel, *sizes),
        (stats, crosses, queries, keys, *back),
        [((rows, ch_dev), BF16)] * 3 + [((ch_dev,), F32)] * 2,
        scratch=[pltpu.VMEM((1, ch_dev), F32)] * 2,
    )
    if query_gain.shape[0] != ch_dev:
        placed = [
            lax.dynamic_update_slice_in_dim(jnp.zeros((channels,), F32), g, start, 0) for g in gain_grads
        ]
        gain_grads = [lax.psum_scatter(g, "fsdp", scatter_dimension=0, tiled=True) for g in placed]
    return (query_grad, key_grad, value_grad, *gain_grads)


def solution(mesh):
    placed = (P("ctx", "fsdp"),) * 6 + (P("fsdp"), P("fsdp"), P(), P("ctx"))
    return jax.shard_map(
        per_device,
        mesh=mesh,
        in_specs=placed,
        out_specs=(P("ctx", "fsdp"), P("ctx", "fsdp"), P("ctx", "fsdp"), P("fsdp"), P("fsdp")),
        check_vma=False,
    )
```

```python
import functools
import math

import jax
import jax.numpy as jnp
import numpy as np
from jax import lax
from jax.experimental import pallas as pl
from jax.experimental.pallas import tpu as pltpu
from jax.sharding import PartitionSpec as P


HD = 128
STEPS = 1000

eps_norm = 1e-06
loss_scale = 256.0
rope_base = 10000.0
floor_term = 0.1

BOTH = ("ctx", "fsdp")
F32 = jnp.float32
BF16 = jnp.bfloat16
ORDER_ROWS = 16

NT = (((1,), (1,)), ((), ()))
TN = (((0,), (0,)), ((), ()))
NN = (((1,), (0,)), ((), ()))


def mm(lhs, rhs, dims):
    return lax.dot_general(lhs, rhs, dims, preferred_element_type=F32)


def eye_mask(size):
    rows = lax.broadcasted_iota(jnp.int32, (size, size), 0)
    return rows == lax.broadcasted_iota(jnp.int32, (size, size), 1)


def as_row(column):
    return jnp.sum(jnp.where(eye_mask(column.shape[0]), column, 0.0), axis=0, keepdims=True)


def columns(rows):
    mask = eye_mask(rows.shape[1])
    return [
        jnp.sum(jnp.where(mask, rows[at : at + 1], 0.0), axis=1, keepdims=True)
        for at in range(rows.shape[0])
    ]


def hosted_head(ctx_id, fsdp_id, n_ctx):
    return (ctx_id + n_ctx - fsdp_id % n_ctx) % n_ctx


def turn(field, cos_t, sin_t):
    return field * cos_t + pltpu.roll(field, HD // 2, 1) * sin_t


def turn_back(field, angles):
    cos_t, sin_t = spread(angles)
    return turn(field, cos_t, -sin_t)


def spread(angles):
    swapped = pltpu.roll(angles, HD // 2, 1)
    low = lax.broadcasted_iota(jnp.int32, angles.shape, 1) < HD // 2
    return jnp.where(low, angles, swapped), jnp.where(low, -swapped, angles)


def head_lanes(head, heads):
    return pl.ds(pl.multiple_of(jnp.minimum(head, heads - 1) * HD, HD), HD)


def norm_scales(stats, channels):
    return lax.rsqrt(stats[0:2] * (1.0 / channels) + eps_norm)


def norm_columns(stats, channels):
    inv = norm_scales(stats, channels)
    tilt = inv * inv * inv * (stats[2:4] * (1.0 / channels))
    return columns(jnp.concatenate([inv, tilt], axis=0))


def pack_kernel(n_ctx, heads, *refs):
    order_hbm, gain_hbms, field_hbms = refs[0], refs[1:3], refs[3:9]
    stats_ref, gain_refs, block_refs = refs[9], refs[10:12], refs[12 : 12 + n_ctx]
    order_ref, line_refs, field_refs, sems = refs[12 + n_ctx], refs[13 + n_ctx : 15 + n_ctx], refs[15 + n_ctx : -1], refs[-1]
    sources = (*field_hbms, order_hbm, *gain_hbms)
    targets = (*field_refs, order_ref, *line_refs)
    copies = [pltpu.make_async_copy(a, b, sems.at[at]) for at, (a, b) in enumerate(zip(sources, targets))]
    for copy in copies:
        copy.start()
    ctx_id, fsdp_id = lax.axis_index("ctx"), lax.axis_index("fsdp")
    rows = field_refs[0].shape[0]
    for copy in copies:
        copy.wait()
    order = jnp.full((ORDER_ROWS, HD), order_ref[0].astype(F32), F32).astype(BF16)
    for dist, block in enumerate(block_refs):
        lanes = head_lanes(hosted_head(ctx_id ^ dist, fsdp_id, n_ctx), heads)
        for at, ref in enumerate(field_refs):
            block[at * rows : (at + 1) * rows, :] = ref[:, lanes]
        block[6 * rows :, :] = order
    q, k, qt, kt = (field_refs[at][...].astype(F32) for at in (0, 1, 3, 4))
    for at, product in enumerate((q * q, k * k, q * qt, k * kt)):
        stats_ref[at : at + 1, :] = as_row(jnp.sum(product, axis=1, keepdims=True))
    for gain_ref, line_ref in zip(gain_refs, line_refs):
        gain_ref[...] = line_ref[...].reshape(gain_ref.shape)


def forward_kernel(n_ctx, n_fsdp, heads, channels, *refs):
    time_ref, gain_q_ref, gain_k_ref, table_ref = refs[:4]
    block_refs = refs[4 : 4 + n_ctx]
    stats_ref = refs[4 + n_ctx]
    energy_ref, qn_ref, kn_ref, vn_ref, x_ref, goal_ref, lse_ref, drift_ref, turn_ref = refs[5 + n_ctx : -5]
    qcat_ref, kcat_ref, vcat_ref, slots_ref, sem = refs[-5:]
    copy = pltpu.make_async_copy(time_ref, slots_ref, sem)
    copy.start()
    ctx_id, fsdp_id = lax.axis_index("ctx"), lax.axis_index("fsdp")
    head = hosted_head(ctx_id, fsdp_id, n_ctx)
    active = head < heads
    lanes = head_lanes(head, heads)
    gain_q, gain_k = gain_q_ref[:, lanes], gain_k_ref[:, lanes]
    rows = (block_refs[0].shape[0] - ORDER_ROWS) // 6
    inv_root = HD ** (-0.5)
    for dist, block in enumerate(block_refs):
        here = slice(dist * rows, (dist + 1) * rows)
        inv_q, inv_k, tilt_q, tilt_k = norm_columns(stats_ref[4 * dist : 4 * dist + 4, :], channels)
        order = block[6 * rows : 6 * rows + 1, :].astype(F32)
        both = table_ref[0:rows, :]
        for other in range(1, n_ctx):
            both = jnp.where(order == float(other), table_ref[other * rows : (other + 1) * rows, :], both)
        turn_ref[here, :] = both
        cos_t, sin_t = spread(both)

        def part(at):
            return block[at * rows : (at + 1) * rows, :]

        q, k = part(0).astype(F32), part(1).astype(F32)
        qt, kt = part(3).astype(F32), part(4).astype(F32)
        qcat_ref[here, HD:] = turn(q * inv_q * gain_q, cos_t, sin_t).astype(BF16)
        qcat_ref[here, 0:HD] = turn((qt * inv_q - q * tilt_q) * gain_q, cos_t, sin_t).astype(BF16)
        kcat_ref[here, 0:HD] = turn(k * inv_k * gain_k, cos_t, sin_t).astype(BF16)
        kcat_ref[here, HD:] = turn((kt * inv_k - k * tilt_k) * gain_k, cos_t, sin_t).astype(BF16)
        vcat_ref[here, 0:HD] = part(2)
        vcat_ref[here, HD:] = part(5)
        vn_ref[here, :] = part(2)
        x_ref[here, 0:HD] = part(0)
        x_ref[here, HD:] = part(1)
    qn_ref[...] = qcat_ref[:, HD:]
    kn_ref[...] = kcat_ref[:, 0:HD]
    copy.wait()
    picked = slots_ref[fsdp_id // (channels // (heads * HD))].astype(F32)
    angle_t = jnp.full((8, HD), 0.5 * math.pi * (picked + 0.5) / STEPS)
    coef_out = (jnp.sin(angle_t) * jnp.cos(angle_t))[0:1]
    coef_tan = (jnp.cos(angle_t) ** 2)[0:1]

    def products(dist):
        here = slice(dist * rows, (dist + 1) * rows)
        return mm(qcat_ref[here, HD:], kcat_ref[:, 0:HD], NT), mm(qcat_ref[here, :], kcat_ref[...], NT)

    later = products(0)
    for dist in range(n_ctx):
        here = slice(dist * rows, (dist + 1) * rows)
        scores, slopes = later
        if dist + 1 < n_ctx:
            later = products(dist + 1)
        peak = jnp.max(scores, axis=1, keepdims=True)
        weights = jnp.exp((scores - peak) * inv_root)
        totals = jnp.sum(weights, axis=1, keepdims=True)
        tilted = weights * slopes
        numer = mm(weights.astype(BF16), vcat_ref[...], NN)
        numer_tan = numer[:, HD:] + inv_root * mm(tilted.astype(BF16), vcat_ref[:, 0:HD], NN)
        tilt = jnp.sum(tilted, axis=1, keepdims=True) * inv_root
        output = numer[:, 0:HD] / totals
        output_tan = (numer_tan - tilt * output) / totals
        goal = coef_out * output + coef_tan * output_tan
        goal_ref[here, :] = goal
        drift_ref[:, here] = as_row(
            jnp.sum(goal.astype(BF16).astype(F32) * output, axis=1, keepdims=True)
        )
        lse_ref[:, here] = as_row(peak * inv_root + jnp.log(totals))
        row = as_row(jnp.sum(goal * goal, axis=1, keepdims=True))
        energy_ref[0, pl.ds(ctx_id ^ dist, 1), :] = jnp.where(active, row, 0.0)
    first = energy_ref[0]
    for at in range(1, energy_ref.shape[0]):
        energy_ref[at] = first


def token_levels(energy_ref, n_ctx, n_fsdp, head_split, channels):
    sample = lax.axis_index("fsdp") // head_split
    energy = sum(
        jnp.sum(energy_ref[pl.ds(at * n_fsdp + sample * head_split, head_split)], axis=0)
        for at in range(n_ctx)
    )
    return loss_scale / (jnp.sqrt(energy * (1.0 / channels)) + floor_term)


def pick_row(table, at):
    ids = lax.broadcasted_iota(jnp.int32, table.shape, 0)
    return jnp.sum(jnp.where(ids == at, table, 0.0), axis=0, keepdims=True)


def query_kernel(n_ctx, heads, channels, *refs):
    gain_ref, qn_ref, kn_ref, vn_ref, x_ref, goal_ref, lse_ref, drift_ref, turn_ref, stats_ref = refs[:10]
    probs_ref, dscore_ref, cross_ref, lift_ref, grown_ref, goal_b_ref, dscore_b_ref = refs[10:]
    head = hosted_head(lax.axis_index("ctx"), lax.axis_index("fsdp"), n_ctx)
    gain = gain_ref[:, head_lanes(head, heads)]
    rows = cross_ref.shape[1]
    inv_root = HD ** (-0.5)
    goal_b_ref[...] = goal_ref[...].astype(BF16)
    blocks = [slice(dist * rows, (dist + 1) * rows) for dist in range(n_ctx)]
    for here in blocks:
        scores = mm(kn_ref[here, :], qn_ref[...], NT)
        probs = jnp.exp(scores * inv_root - lse_ref[...])
        dprobs = mm(vn_ref[here, :], goal_b_ref[...], NT)
        dscore = probs * (dprobs - drift_ref[...])
        probs_ref[here, :] = probs.astype(BF16)
        dscore_ref[here, :] = dscore
        dscore_b_ref[here, :] = dscore.astype(BF16)
    for dist, here in enumerate(blocks):
        dquery = mm(dscore_b_ref[:, here], kn_ref[...], TN) * inv_root
        (inv_q,) = columns(norm_scales(stats_ref[4 * dist : 4 * dist + 4, :], channels)[0:1])
        x = x_ref[here, 0:HD].astype(F32)
        dy = turn_back(dquery, turn_ref[here, :])
        grown = gain * dy
        grown_ref[here, :] = grown
        cross_ref[dist : dist + 1, :] = as_row(jnp.sum(x * grown, axis=1, keepdims=True))
        lift_ref[here, :] = dy * x * inv_q


def key_kernel(n_ctx, n_fsdp, heads, channels, *refs):
    energy_ref, gain_ref, qn_ref, x_ref, goal_ref, turn_ref, stats_ref = refs[:7]
    probs_ref, dscore_ref, cross_q_ref, lift_ref, grown_ref, cross_ref = refs[7:13]
    back_refs = refs[13 : 13 + n_ctx]
    cot_ref = refs[13 + n_ctx]
    ctx_id, fsdp_id = lax.axis_index("ctx"), lax.axis_index("fsdp")
    head = hosted_head(ctx_id, fsdp_id, n_ctx)
    active = head < heads
    gain = gain_ref[:, head_lanes(head, heads)]
    rows = cross_q_ref.shape[1]
    level = token_levels(energy_ref, n_ctx, n_fsdp, channels // (heads * HD), channels)
    levels = [pick_row(level, ctx_id ^ dist) for dist in range(n_ctx)]
    blocks = [slice(dist * rows, (dist + 1) * rows) for dist in range(n_ctx)]
    gain_q_sum = jnp.zeros((1, HD), F32)
    for here, row, back in zip(blocks, levels, back_refs):
        (scale,) = columns(row)
        back[0:rows, :] = (scale * grown_ref[here, :]).astype(BF16)
        cot_ref[here, :] = (scale * goal_ref[here, :]).astype(BF16)
        gain_q_sum = gain_q_sum + jnp.sum(scale * lift_ref[here, :], axis=0, keepdims=True)
    level_row = jnp.concatenate(levels, axis=1) * HD ** (-0.5)
    gain_k_sum = jnp.zeros((1, HD), F32)
    cross_k = []
    for dist, here in enumerate(blocks):
        back_refs[dist][2 * rows :, :] = mm(probs_ref[here, :], cot_ref[...], NN).astype(BF16)
        dscore = (dscore_ref[here, :] * level_row).astype(BF16)
        dkey = mm(dscore, qn_ref[...], NN)
        (inv_k,) = columns(norm_scales(stats_ref[4 * dist : 4 * dist + 4, :], channels)[1:2])
        x = x_ref[here, HD:].astype(F32)
        dy = turn_back(dkey, turn_ref[here, :])
        grown = gain * dy
        back_refs[dist][rows : 2 * rows, :] = grown.astype(BF16)
        cross_k.append(as_row(jnp.sum(x * grown, axis=1, keepdims=True)))
        gain_k_sum = gain_k_sum + jnp.sum(dy * x * inv_k, axis=0, keepdims=True)
    for dist in range(n_ctx):
        cross_q = cross_q_ref[dist : dist + 1, :] * levels[dist]
        sums = jnp.concatenate([cross_q, cross_k[dist], gain_q_sum, gain_k_sum], axis=0)
        sums = jnp.where(active, sums, 0.0)
        start = (ctx_id ^ dist) * n_fsdp
        for at in range(n_fsdp):
            cross_ref[start + at] = sums


def finish_kernel(n_ctx, n_fsdp, heads, channels, *refs):
    stats_ref, cross_ref, q_ref, k_ref = refs[:4]
    back_refs = refs[4 : 4 + n_ctx]
    dq_ref, dk_ref, dv_ref, dgain_q_ref, dgain_k_ref, gain_q_ref, gain_k_ref = refs[4 + n_ctx :]
    ctx_id, fsdp_id = lax.axis_index("ctx"), lax.axis_index("fsdp")
    head_split = channels // (heads * HD)
    sample = fsdp_id // head_split
    rows = q_ref.shape[0]
    inv = norm_scales(stats_ref[0:4, :], channels)
    total = jnp.zeros((4, rows), F32)
    for ctx_at in range(n_ctx):
        total = total + jnp.sum(cross_ref[pl.ds(ctx_at * n_fsdp + sample * head_split, head_split)], axis=0)
    tilt = inv * inv * inv * (total[0:2] * (1.0 / channels))
    inv_q, inv_k, tilt_q, tilt_k = columns(jnp.concatenate([inv, tilt], axis=0))
    for dist in range(n_ctx):
        host = ctx_id ^ dist
        head = hosted_head(host, fsdp_id, n_ctx)

        @pl.when(head < heads)
        def _(dist=dist, host=host, head=head):
            back = back_refs[dist]
            lanes = head_lanes(head, heads)
            h_q, h_k = back[0:rows, :].astype(F32), back[rows : 2 * rows, :].astype(F32)
            dq_ref[:, lanes] = (inv_q * h_q - q_ref[:, lanes].astype(F32) * tilt_q).astype(BF16)
            dk_ref[:, lanes] = (inv_k * h_k - k_ref[:, lanes].astype(F32) * tilt_k).astype(BF16)
            dv_ref[:, lanes] = back[2 * rows :, :]
            sums = cross_ref[host * n_fsdp + fsdp_id]
            gain_q_ref[:, lanes] = sums[2:3]
            gain_k_ref[:, lanes] = sums[3:4]

    dgain_q_ref[...] = gain_q_ref[...].reshape(dgain_q_ref.shape)
    dgain_k_ref[...] = gain_k_ref[...].reshape(dgain_k_ref.shape)


def per_device(
    queries,
    keys,
    values,
    query_tangent,
    key_tangent,
    value_tangent,
    query_gain,
    key_gain,
    time_index,
    shard_order,
):
    n_ctx, n_fsdp = lax.axis_size("ctx"), lax.axis_size("fsdp")
    n_all = n_ctx * n_fsdp
    fsdp_id = lax.axis_index("fsdp")
    rows, ch_dev = queries.shape
    heads = ch_dev // HD
    channels = query_gain.shape[0] * n_fsdp
    head_split = channels // ch_dev
    seq = rows * n_ctx
    sizes = (n_ctx, n_fsdp, heads, channels)

    vmem = pl.BlockSpec(memory_space=pltpu.VMEM)

    hbm = pl.BlockSpec(memory_space=pltpu.HBM)

    def kernel(body, ins, outs, scratch=(), flops=10**8, from_hbm=0):
        return pl.pallas_call(
            body,
            out_shape=[jax.ShapeDtypeStruct(*o) for o in outs],
            in_specs=[hbm] * from_hbm + [vmem] * (len(ins) - from_hbm),
            out_specs=[vmem] * len(outs),
            scratch_shapes=list(scratch),
            cost_estimate=pl.CostEstimate(flops=flops, bytes_accessed=2**20, transcendentals=0),
            compiler_params=pltpu.CompilerParams(vmem_limit_bytes=16 * 2**20 + seq * 2**14),
        )(*ins)

    def in_hbm(array):
        return pltpu.with_memory_space_constraint(array, pltpu.HBM)

    def swap(block, axis, dist):
        return lax.ppermute(block, axis, [(i, i ^ dist) for i in range(lax.axis_size(axis))])

    def sum_over_sample(block):
        block = block + swap(block, "fsdp", 1)
        return sum([swap(block, "fsdp", d) for d in range(2, head_split, 2)], block)

    def from_peers(blocks, idle=None):
        out = [blocks[0]] + [None] * (n_ctx - 1)
        for dist in reversed(range(1, n_ctx)):
            route = []
            for c in range(n_ctx):
                for f in range(n_fsdp):
                    near = idle and idle(c, c ^ dist, f) and idle(c ^ dist, c, f ^ 1)
                    target = (c, f ^ 1) if near else (c ^ dist, f)
                    route.append((c * n_fsdp + f, target[0] * n_fsdp + target[1]))
            out[dist] = lax.ppermute(blocks[dist], BOTH, route)
        return out

    places = np.arange(seq, dtype=np.float32)
    freqs = (rope_base ** (-np.arange(HD // 2) / (HD // 2))).astype(np.float32)
    angles = (places[:, None] * freqs[None, :]).astype(np.float64)
    table = jnp.asarray(np.concatenate([np.cos(angles), np.sin(angles)], axis=1).astype(np.float32))

    gains = (query_gain, key_gain)
    if query_gain.shape[0] != ch_dev:
        start = (fsdp_id % head_split) * ch_dev
        gains = [lax.all_gather(g, "fsdp", axis=0, tiled=True) for g in gains]
        gains = [lax.dynamic_slice_in_dim(g, start, ch_dev, 0) for g in gains]

    fields = (queries, keys, values, query_tangent, key_tangent, value_tangent)
    gains = [in_hbm(a) for a in gains]
    fields = [in_hbm(a) for a in fields]
    part, gain_q, gain_k, *blocks = kernel(
        functools.partial(pack_kernel, n_ctx, heads),
        (shard_order, *gains, *fields),
        [((4, rows), F32)] + [((1, ch_dev), F32)] * 2 + [((6 * rows + ORDER_ROWS, HD), BF16)] * n_ctx,
        scratch=[pltpu.SMEM((1,), jnp.int32)]
        + [pltpu.VMEM((ch_dev,), F32)] * 2
        + [pltpu.VMEM((rows, ch_dev), BF16)] * 6
        + [pltpu.SemaphoreType.DMA((9,))],
        from_hbm=9,
    )
    gains = (gain_q, gain_k)
    parts = from_peers([part] * n_ctx)
    blocks = from_peers(blocks, lambda c, peer, f: hosted_head(peer, f, n_ctx) >= heads)
    stats = sum_over_sample(jnp.concatenate(parts, axis=0))

    energy_out, qn, kn, vn, x, goal, lse, drift, turns = kernel(
        functools.partial(forward_kernel, *sizes),
        (time_index, *gains, table, *blocks, stats),
        [((n_all, n_ctx, rows), F32)]
        + [((seq, HD), BF16)] * 3
        + [((seq, 2 * HD), BF16), ((seq, HD), F32)]
        + [((1, seq), F32)] * 2
        + [((seq, HD), F32)],
        scratch=[pltpu.VMEM((seq, 2 * HD), BF16)] * 3
        + [pltpu.SMEM(time_index.shape, jnp.int32), pltpu.SemaphoreType.DMA],
        from_hbm=1,
    )
    energy = lax.all_to_all(energy_out, BOTH, 0, 0)
    probs, dscore, cross_q, lift, grown = kernel(
        functools.partial(query_kernel, n_ctx, heads, channels),
        (gain_q, qn, kn, vn, x, goal, lse, drift, turns, stats),
        [((seq, seq), BF16), ((seq, seq), F32), ((n_ctx, rows), F32)] + [((seq, HD), F32)] * 2,
        scratch=[pltpu.VMEM((seq, HD), BF16), pltpu.VMEM((seq, seq), BF16)],
    )

    cross_out, *back = kernel(
        functools.partial(key_kernel, *sizes),
        (energy, gain_k, qn, x, goal, turns, stats, probs, dscore, cross_q, lift, grown),
        [((n_all, 4, rows), F32)] + [((3 * rows, HD), BF16)] * n_ctx,
        scratch=[pltpu.VMEM((seq, HD), BF16)],
    )
    back = from_peers(back, lambda c, peer, f: hosted_head(c, f, n_ctx) >= heads)
    crosses = lax.all_to_all(cross_out, BOTH, 0, 0)

    query_grad, key_grad, value_grad, *gain_grads = kernel(
        functools.partial(finish_kernel, *sizes),
        (stats, crosses, queries, keys, *back),
        [((rows, ch_dev), BF16)] * 3 + [((ch_dev,), F32)] * 2,
        scratch=[pltpu.VMEM((1, ch_dev), F32)] * 2,
    )
    if query_gain.shape[0] != ch_dev:
        placed = [
            lax.dynamic_update_slice_in_dim(jnp.zeros((channels,), F32), g, start, 0) for g in gain_grads
        ]
        gain_grads = [lax.psum_scatter(g, "fsdp", scatter_dimension=0, tiled=True) for g in placed]
    return (query_grad, key_grad, value_grad, *gain_grads)


def solution(mesh):
    placed = (P("ctx", "fsdp"),) * 6 + (P("fsdp"), P("fsdp"), P(), P("ctx"))
    return jax.shard_map(
        per_device,
        mesh=mesh,
        in_specs=placed,
        out_specs=(P("ctx", "fsdp"), P("ctx", "fsdp"), P("ctx", "fsdp"), P("fsdp"), P("fsdp")),
        check_vma=False,
    )
```
